256 devices in a mesh: band: 128 (over z, y, x), ch: 2 (over core).
Axes of the slice: x: 4, y: 4, z: 8, core: 2. Of those that a mesh axis runs over, the one named last changes fastest.
Arguments:
- grid_field: bfloat16 [100, 2097152], P(None, 'band'), may hold values from -6 to 6
- band_points: int32 [128], P('band'), may hold values from 8192 to 16384
- block_ids: int32 [128, 16], P('band'), may hold values from 0 to 4095, as said below
- block_count: int32 [128], P('band'), may hold values from 8 to 16
- block_weight: bfloat16 [128, 16, 256, 512], P('band'), may hold values from 0 to 0.039794922
- embed_weight: bfloat16 [100, 1024], P(None, 'ch'), may hold values from -0.3125 to 0.3125
- edge_src: int32 [655360], P('band'), may hold values from 0 to 32767, as said below
- edge_dst: int32 [655360], P('band'), may hold values from 0 to 32767, as said below
- edge_in_weight: bfloat16 [2, 1024, 1024], P(None, None, 'ch'), may hold values from -0.1875 to 0.1875
- edge_out_weight: bfloat16 [1024, 1024], P('ch'), may hold values from -0.0625 to 0.0625
- node_in_weight: bfloat16 [2, 1024, 1024], P(None, None, 'ch'), may hold values from -0.125 to 0.125
- node_out_weight: bfloat16 [1024, 1024], P('ch'), may hold values from -0.1875 to 0.1875
Outputs:
- node_state: bfloat16 [32768, 1024], P('band', 'ch')
The draws below stay inside these ranges and needn't reach their ends.
Inputs may be any that keep to these rules, and one draw needn't show every extreme that they name: For band b, block_ids[b, k] * 512 lies from max(b * 16384 - 16384 // 2, 0) to min((b + 1) * 16384 + 16384 // 2, 2097152) - 512; both ends are named by every band; ids may repeat. `edge_src`: edge e belongs to band b = e // 5120; its source node lies in bands b - 1 to b + 1 of the mesh. `edge_dst`: edge e ends at a node of its band b = e // 5120.
All inputs are finite; a program needn't handle non-finite values.
Results may differ from the reference program's by a relative error of at most 0.015.
Values may be sent and summed in bfloat16 or wider, within the bound.
A program may use at most 64 MiB of HBM per device.

```python
import jax
import jax.numpy as jnp
from jax import lax

CIN = 100
H = 1024
PTS_DEV = 16384
NODE_DEV = 256
E_DEV = 5120
PBLK = 512
K = 16
POINTS = 2097152
NODES = 32768
EDGES = 655360
N_BAND = 128


def draw_block_ids(key, part):
    sub_count = PTS_DEV // PBLK
    band_index = jnp.arange(N_BAND, dtype=jnp.int32)[:, None]
    lowest = jnp.maximum(band_index * sub_count - sub_count // 2, 0)
    highest = jnp.minimum((band_index + 1) * sub_count + sub_count // 2, N_BAND * sub_count)
    raw_bits = jax.random.randint(jax.random.fold_in(key, 11), (N_BAND, K), 0, 1 << 30)
    picked = lowest + raw_bits % (highest - lowest)
    slot_index = jnp.arange(K, dtype=jnp.int32)[None, :]
    picked = jnp.where(slot_index == 0, lowest, picked)
    picked = jnp.where(slot_index == 1, highest - 1, picked)
    return picked.astype(jnp.int32)


def draw_edge_src(key, part):
    edge_index = jnp.arange(EDGES, dtype=jnp.int32)
    band_index = edge_index // E_DEV
    lowest = jnp.maximum(band_index - 1, 0) * NODE_DEV
    highest = jnp.minimum(band_index + 2, N_BAND) * NODE_DEV
    return jax.random.randint(jax.random.fold_in(key, 21), (EDGES,), lowest, highest).astype(jnp.int32)


def draw_edge_dst(key, part):
    edge_index = jnp.arange(EDGES, dtype=jnp.int32)
    band_index = edge_index // E_DEV
    offset = jax.random.randint(jax.random.fold_in(key, 31), (EDGES,), 0, NODE_DEV)
    return (band_index * NODE_DEV + offset).astype(jnp.int32)


def set_ends(drawn, rng, low, high):
    spot = [jax.random.randint(jax.random.fold_in(rng, axis), (), 0, length) for axis, length in enumerate(drawn.shape)]
    longest = drawn.shape.index(max(drawn.shape))
    neighbour = spot[:longest] + [(spot[longest] + 1) % drawn.shape[longest]] + spot[longest + 1:]
    return drawn.at[tuple(spot)].set(low).at[tuple(neighbour)].set(high)


def block_levels(stream_key, extent, shards, low, top_value):
    level, own = 1.0, jax.random.fold_in(stream_key, 6)
    for dim, parts in shards:
        draws = jnp.exp(jax.random.uniform(jax.random.fold_in(own, dim), (parts,), jnp.float32, low / len(shards), top_value / len(shards)))
        level = level * jnp.repeat(draws, extent[dim] // parts).reshape([-1 if axis == dim else 1 for axis in range(len(extent))])
    return level


def bell_draw(stream_key, dims, scale, most, split=(), kind=jnp.bfloat16):
    entries = jax.random.normal(stream_key, dims, jnp.float32) * scale
    if len(split) > 0:
        entries = block_levels(stream_key, dims, split, -0.22, 0.18) * entries
    return jnp.clip(entries, min=-most, max=most).astype(kind)


def setup_inputs(seed: int = 0) -> dict:
    streams_of = jax.random.split(jax.random.key(seed), 13)
    grid_field = bell_draw(streams_of[0], (CIN, POINTS), 1.0, 6.0, ((1, 128),))
    band_points = set_ends(jax.random.randint(streams_of[1], (N_BAND,), PTS_DEV // 2, PTS_DEV + 1), jax.random.fold_in(streams_of[1], 1), PTS_DEV // 2, PTS_DEV).astype(jnp.int32)
    block_ids = draw_block_ids(jax.random.fold_in(streams_of[12], 71), 0)
    block_count = set_ends(jax.random.randint(streams_of[3], (N_BAND,), K // 2, K + 1), jax.random.fold_in(streams_of[3], 1), K // 2, K).astype(jnp.int32)
    block_weight = jnp.clip(0.039794922 * jax.random.uniform(streams_of[4], (N_BAND, K, NODE_DEV, PBLK), jnp.float32) ** block_levels(streams_of[4], (N_BAND, K, NODE_DEV, PBLK), ((0, 128),), -0.2, 0.2), 0.0, 0.039794922).astype(jnp.bfloat16)
    embed_weight = bell_draw(streams_of[5], (CIN, H), (4 * CIN) ** -0.5, 0.3125, ((1, 2),))
    edge_src = draw_edge_src(jax.random.fold_in(streams_of[12], 71), 0)
    edge_dst = draw_edge_dst(jax.random.fold_in(streams_of[12], 71), 0)
    edge_in_weight = bell_draw(streams_of[8], (2, H, H), H ** -0.5, 0.1875, ((2, 2),))
    edge_out_weight = bell_draw(streams_of[9], (H, H), (8 * H) ** -0.5, 0.0625, ((0, 2),))
    node_in_weight = bell_draw(streams_of[10], (2, H, H), (2 * H) ** -0.5, 0.125, ((2, 2),))
    node_out_weight = bell_draw(streams_of[11], (H, H), H ** -0.5, 0.1875, ((0, 2),))
    return {"grid_field": grid_field, "band_points": band_points, "block_ids": block_ids, "block_count": block_count, "block_weight": block_weight, "embed_weight": embed_weight, "edge_src": edge_src, "edge_dst": edge_dst, "edge_in_weight": edge_in_weight, "edge_out_weight": edge_out_weight, "node_in_weight": node_in_weight, "node_out_weight": node_out_weight}


def reference(grid_field, band_points, block_ids, block_count, block_weight, embed_weight, edge_src, edge_dst, edge_in_weight, edge_out_weight, node_in_weight, node_out_weight):
    column = jnp.arange(POINTS, dtype=jnp.int32)
    limit = band_points[column // PTS_DEV]
    live = jnp.where((column % PTS_DEV < limit)[None, :], grid_field, jnp.zeros_like(grid_field))
    tiles = live.reshape(CIN, POINTS // PBLK, PBLK)

    def remap_band(inputs):
        ids, count, weights = inputs
        blocks = jnp.take(tiles, ids, axis=1)
        live_mask = jnp.arange(K, dtype=jnp.int32) < count
        blocks = jnp.where(live_mask[None, :, None], blocks, jnp.zeros_like(blocks))
        summed = jnp.einsum("knp,ckp->nc", weights.astype(jnp.float32), blocks.astype(jnp.float32))
        return summed.astype(jnp.bfloat16)

    remapped = lax.map(remap_band, (block_ids, block_count, block_weight)).reshape(NODES, CIN)
    initial = jnp.dot(remapped, embed_weight, preferred_element_type=jnp.float32).astype(jnp.bfloat16)
    source_proj = jnp.dot(initial, edge_in_weight[0], preferred_element_type=jnp.float32).astype(jnp.bfloat16)
    target_proj = jnp.dot(initial, edge_in_weight[1], preferred_element_type=jnp.float32).astype(jnp.bfloat16)

    def band_messages(inputs):
        sources, targets = inputs
        pre_act = jnp.take(source_proj, sources, axis=0).astype(jnp.float32) + jnp.take(target_proj, targets, axis=0).astype(jnp.float32)
        edge_hidden = jax.nn.silu(pre_act).astype(jnp.bfloat16)
        messages = jnp.dot(edge_hidden, edge_out_weight, preferred_element_type=jnp.float32)
        return jax.ops.segment_sum(messages, targets % NODE_DEV, num_segments=NODE_DEV)

    aggregate = lax.map(band_messages, (edge_src.reshape(N_BAND, E_DEV), edge_dst.reshape(N_BAND, E_DEV)))
    aggregate = aggregate.reshape(NODES, H).astype(jnp.bfloat16)
    inner = jnp.dot(initial, node_in_weight[0], preferred_element_type=jnp.float32) + jnp.dot(aggregate, node_in_weight[1], preferred_element_type=jnp.float32)
    update = jax.nn.silu(inner).astype(jnp.bfloat16)
    result = initial.astype(jnp.float32) + jnp.dot(update, node_out_weight, preferred_element_type=jnp.float32)
    return result.astype(jnp.bfloat16)
```

```python
import functools

import jax
import jax.numpy as jnp
from jax import lax
from jax.experimental import pallas as pl
from jax.experimental.pallas import tpu as pltpu
from jax.sharding import PartitionSpec as P

MESH = pl.DeviceIdType.MESH
F32 = jnp.float32
BF16 = jnp.bfloat16
VMEM = pl.BlockSpec(memory_space=pltpu.VMEM)
SMEM = pl.BlockSpec(memory_space=pltpu.SMEM)
HBM = pl.BlockSpec(memory_space=pltpu.HBM)
LARGE = 48 * 1024 * 1024
CHUNK = 512
PAD = 128


def nt(x, y):
    return lax.dot_general(x, y, (((1,), (1,)), ((), ())), preferred_element_type=F32)


def mm(x, y):
    return jnp.dot(x, y, preferred_element_type=F32)


def silu_of_half(v):
    return v + v * jnp.tanh(v)


def layer_kernel(
    n, ids, count, live, grid_h, w_h, emb_h, eo_h, win_h, nin_h, nout_h, src_h, dst_h, out,
    pool, wts, emb, embp, eo, win, nin, nout, nout_o, src, dst,
    mt, dmix, pmix, hs, hd, part, other, ext, near, gown, gdst, acc, agg, agg_o, upd, upd_o,
    wsem, gsem, lsem, send, recv,
):
    b = lax.axis_index("band")
    c = lax.axis_index("ch")
    slots, nodes, block_len = w_h.shape
    width = block_len // 2
    channels = grid_h.shape[0]
    sub = grid_h.shape[1] // block_len
    half = sub // 2
    cols = emb_h.shape[1]
    hid = 2 * cols
    mine_e = src.shape[1]
    chunks = mine_e // CHUNK
    dead = 2 * sub
    up, down = jnp.minimum(b + 1, n - 1), jnp.maximum(b - 1, 0)
    has_up, has_down = b < n - 1, b > 0
    above, below, partner = (up, c), (down, c), (b, 1 - c)

    ext[...] = jnp.zeros_like(ext)
    barrier = pltpu.get_barrier_semaphore()
    pl.semaphore_signal(barrier, inc=1, device_id=partner, device_id_type=MESH)

    @pl.when(has_up)
    def _():
        pl.semaphore_signal(barrier, inc=1, device_id=above, device_id_type=MESH)

    @pl.when(has_down)
    def _():
        pl.semaphore_signal(barrier, inc=1, device_id=below, device_id_type=MESH)

    off = pl.multiple_of(c * width, width)
    gcopies = [
        pltpu.make_async_copy(
            grid_h.at[:, pl.ds(pl.multiple_of((2 * i + c) * width, width), width)], pool.at[half + i], gsem.at[i]
        )
        for i in range(sub)
    ]
    wcopies = [
        pltpu.make_async_copy(w_h.at[k, :, pl.ds(off, width)], wts.at[:, pl.ds(k * width, width)], wsem.at[k])
        for k in range(slots)
    ]
    mine = pl.ds(pl.multiple_of(c * cols, cols), cols)
    theirs = pl.ds(pl.multiple_of((1 - c) * cols, cols), cols)
    edges = pl.ds(pl.multiple_of(c * mine_e, mine_e), mine_e)
    local = [
        pltpu.make_async_copy(x, y, lsem.at[i])
        for i, (x, y) in enumerate(
            [(emb_h, emb.at[c]), (win_h, win), (eo_h, eo.at[c]), (nin_h, nin), (nout_h.at[:, mine], nout),
             (src_h.at[:, edges], src), (dst_h.at[:, edges], dst)]
        )
    ]
    for one in gcopies[half:] + gcopies[:half] + local + wcopies:
        one.start()

    def remote(source, target, k, device):
        return pltpu.make_async_remote_copy(
            src_ref=source, dst_ref=target, send_sem=send.at[k], recv_sem=recv.at[k],
            device_id=device, device_id_type=MESH,
        )

    def neighbours(fwd, bwd):
        def end():
            @pl.when(has_up)
            def _():
                fwd.wait_send()
                bwd.wait_recv()

            @pl.when(has_down)
            def _():
                bwd.wait_send()
                fwd.wait_recv()

        return (lambda: pl.when(has_up)(fwd.start)), (lambda: pl.when(has_down)(bwd.start)), end

    halo_up, halo_down, halo_end = neighbours(
        remote(pool.at[pl.ds(sub, half)], pool.at[pl.ds(0, half)], 0, above),
        remote(pool.at[pl.ds(half, half)], pool.at[pl.ds(half + sub, half)], 1, below),
    )
    rows_up, rows_down, rows_end = neighbours(
        remote(ext.at[1], ext.at[0], 7, above), remote(ext.at[1], ext.at[2], 8, below)
    )
    weights = [
        remote(emb_h, emb.at[c], 2, partner), remote(eo_h, eo.at[c], 3, partner),
        remote(nout_h.at[:, theirs], nout_o, 4, partner),
    ]

    for one in gcopies:
        one.wait()
    column = lax.broadcasted_iota(jnp.int32, (channels, width), 1) + c * width
    for i in range(half, sub):
        block = pool[half + i]
        pool[half + i] = jnp.where(column < live[0] - i * block_len, block, jnp.zeros_like(block))
    pool[dead] = jnp.zeros((channels, width), BF16)

    @pl.when(b == 0)
    def _():
        pool[0:half] = jnp.zeros((half, channels, width), BF16)

    @pl.when(b == n - 1)
    def _():
        pool[half + sub:dead] = jnp.zeros((half, channels, width), BF16)

    pl.semaphore_wait(barrier, 1 + has_up.astype(jnp.int32) + has_down.astype(jnp.int32))
    halo_up()
    halo_down()
    for one in weights:
        one.start()

    for one in local + weights:
        one.wait()
    embp[...] = jnp.zeros_like(embp)
    embp[0:channels, 0:cols] = emb[0]
    embp[0:channels, cols:hid] = emb[1]
    for i in range(2):
        mixed = mm(embp[...], win[i]) * 0.5
        mt[mine, i * PAD:(i + 1) * PAD] = mixed.T.astype(BF16)
    share = remote(mt.at[mine], mt.at[mine], 5, partner)
    share.start()
    dmix[...] = mm(embp[...], nin[0]).astype(BF16)
    for i in range(2):
        pmix[i * cols:(i + 1) * cols, :] = mm(eo[i], nin[1]).astype(BF16)

    def hot(i, carry):
        at = pl.ds(pl.multiple_of(i * CHUNK, CHUNK), CHUNK)
        s = src[:, at] - (b - 1) * nodes
        s = jnp.where(s < nodes, s, jnp.where(s < 2 * nodes, s + nodes, s - nodes))
        d = dst[:, at] - b * nodes
        hs[:, at] = jnp.where(lax.broadcasted_iota(jnp.int32, (3 * nodes, CHUNK), 0) == s, 1.0, 0.0).astype(BF16)
        hd[:, at] = jnp.where(lax.broadcasted_iota(jnp.int32, (nodes, CHUNK), 0) == d, 1.0, 0.0).astype(BF16)
        return carry

    lax.fori_loop(0, chunks, hot, 0)
    acc[...] = jnp.zeros_like(acc)
    part[...] = jnp.zeros_like(part)
    share.wait()
    for one in wcopies:
        one.wait()
    halo_end()

    picked = []
    for k in range(slots):
        rel = jnp.clip(ids[0, k] - b * sub + half, 0, dead - 1)
        picked.append(pool[jnp.where(k < count[0], rel, dead)])
    part[0:channels, :] = nt(jnp.concatenate(picked, axis=1), wts[...])
    swap = remote(part, other, 6, partner)
    swap.start()
    swap.wait()
    own = (part[...] + other[...]).astype(BF16)
    ext[1] = own
    rows_up()
    rows_down()

    rows = own.astype(F32).T.astype(BF16)
    first = mm(rows, embp[:, mine]).astype(BF16).astype(F32)
    inner = mm(rows, dmix[...])
    gdst[...] = mm(own, hd[...]).astype(BF16)
    gown[...] = mm(own, hs[2 * nodes:, :]).astype(BF16)
    rows_end()
    near[:, 0:nodes] = ext[0]
    near[:, nodes:] = ext[2]

    def step(i, carry):
        at = pl.ds(pl.multiple_of(i * CHUNK, CHUNK), CHUNK)
        gsrc = (mm(near[...], hs[0:2 * nodes, at]) + gown[:, at].astype(F32)).astype(BF16)
        pre = mm(mt[...], jnp.concatenate([gsrc, gdst[:, at]], axis=0))
        hidden = silu_of_half(pre).astype(BF16)
        acc[...] += nt(hd[:, at], hidden)
        return carry

    lax.fori_loop(0, chunks, step, 0, unroll=True)
    agg[...] = acc[...].astype(BF16)
    swap = remote(agg, agg_o, 9, partner)
    swap.start()
    inner += mm(agg[...], pmix[...])
    swap.wait()
    inner = 0.5 * (inner + mm(agg_o[...], pmix[...]))
    upd[...] = silu_of_half(inner).astype(BF16)
    last = remote(upd, upd_o, 10, partner)
    last.start()
    kept = first + mm(upd[...], nout[...])
    last.wait()
    out[...] = (kept + mm(upd_o[...], nout_o[...])).astype(BF16)


def on_device(
    grid_field, band_points, block_ids, block_count, block_weight, embed_weight,
    edge_src, edge_dst, edge_in_weight, edge_out_weight, node_in_weight, node_out_weight,
):
    n = lax.axis_size("band")
    channels, points = grid_field.shape
    slots, nodes, block_len = block_weight.shape[1:]
    sub = points // block_len
    width = block_len // 2
    cols = embed_weight.shape[1]
    hid = 2 * cols
    edges = edge_src.shape[0] // 2
    bf = lambda *shape: pltpu.VMEM(shape, BF16)
    f32 = lambda *shape: pltpu.VMEM(shape, F32)
    return pl.pallas_call(
        functools.partial(layer_kernel, n),
        out_shape=jax.ShapeDtypeStruct((nodes, cols), BF16),
        in_specs=[SMEM] * 3 + [HBM] * 9, out_specs=VMEM,
        scratch_shapes=[
            bf(2 * sub + 1, channels, width), bf(nodes, slots * width),
            bf(2, channels, cols), bf(PAD, hid), bf(2, cols, hid), bf(2, hid, cols), bf(2, hid, cols),
            bf(cols, cols), bf(cols, cols),
            pltpu.VMEM((1, edges), jnp.int32), pltpu.VMEM((1, edges), jnp.int32),
            bf(hid, 2 * PAD), bf(PAD, cols), bf(hid, cols), bf(3 * nodes, edges), bf(nodes, edges),
            f32(PAD, nodes), f32(PAD, nodes), bf(3, PAD, nodes), bf(PAD, 2 * nodes),
            bf(PAD, edges), bf(PAD, edges), f32(nodes, hid),
            bf(nodes, hid), bf(nodes, hid), bf(nodes, cols), bf(nodes, cols),
            pltpu.SemaphoreType.DMA((slots,)), pltpu.SemaphoreType.DMA((sub,)), pltpu.SemaphoreType.DMA((7,)),
            pltpu.SemaphoreType.DMA((11,)), pltpu.SemaphoreType.DMA((11,)),
        ],
        compiler_params=pltpu.CompilerParams(vmem_limit_bytes=LARGE, collective_id=0, has_side_effects=True),
    )(
        block_ids, block_count, band_points, grid_field, block_weight.reshape(block_weight.shape[1:]),
        embed_weight, edge_out_weight, edge_in_weight, node_in_weight, node_out_weight,
        edge_src.reshape(1, -1), edge_dst.reshape(1, -1),
    )


def solution(mesh):
    return jax.shard_map(
        on_device,
        mesh=mesh,
        in_specs=(
            P(None, "band"), P("band"), P("band", None), P("band"),
            P("band", None, None, None), P(None, "ch"), P("band"), P("band"),
            P(None, None, "ch"), P("ch", None), P(None, None, "ch"), P("ch", None),
        ),
        out_specs=P("band", "ch"),
        check_vma=False,
    )
```

```python
import functools

import jax
import jax.numpy as jnp
from jax import lax
from jax.experimental import pallas as pl
from jax.experimental.pallas import tpu as pltpu
from jax.sharding import PartitionSpec as P

MESH = pl.DeviceIdType.MESH
F32 = jnp.float32
BF16 = jnp.bfloat16
VMEM = pl.BlockSpec(memory_space=pltpu.VMEM)
SMEM = pl.BlockSpec(memory_space=pltpu.SMEM)
HBM = pl.BlockSpec(memory_space=pltpu.HBM)
LARGE = 63 * 1024 * 1024
CHUNK = 512
PAD = 128
ROWS = 112


def nt(x, y):
    return lax.dot_general(x, y, (((1,), (1,)), ((), ())), preferred_element_type=F32)


def mm(x, y):
    return jnp.dot(x, y, preferred_element_type=F32)


def silu_of_half(v):
    return v + v * jnp.tanh(v)


def layer_kernel(
    n, ids, count, live, grid_h, w_h, emb_h, eo_h, win_h, nin_h, nout_h, src_h, dst_h, out,
    pool, wts, wt, emb, embp, eo, win, nin, nout, src, dst,
    mt, dmix, pmix, hs, hd, part, other, ext, near, gown, gath, acc, give, take, fin,
    wsem, gsem, lsem, send, recv,
):
    b = lax.axis_index("band")
    c = lax.axis_index("ch")
    slots, nodes, block_len = w_h.shape
    width = block_len // 2
    channels = grid_h.shape[0]
    sub = grid_h.shape[1] // block_len
    half = sub // 2
    cols = emb_h.shape[1]
    hid = 2 * cols
    mine_e = src.shape[1]
    chunks = mine_e // CHUNK
    mid = nodes // 2
    dead = 2 * sub
    up, down = jnp.minimum(b + 1, n - 1), jnp.maximum(b - 1, 0)
    has_up, has_down = b < n - 1, b > 0
    above, below, partner = (up, c), (down, c), (b, 1 - c)

    ext[...] = jnp.zeros_like(ext)
    barrier = pltpu.get_barrier_semaphore()

    @pl.when(has_up)
    def _():
        pl.semaphore_signal(barrier, inc=1, device_id=above, device_id_type=MESH)

    @pl.when(has_down)
    def _():
        pl.semaphore_signal(barrier, inc=1, device_id=below, device_id_type=MESH)

    pl.semaphore_signal(barrier, inc=1, device_id=partner, device_id_type=MESH)

    off = pl.multiple_of(c * width, width)
    gcopies = [
        pltpu.make_async_copy(
            grid_h.at[:, pl.ds(pl.multiple_of((2 * i + c) * width, width), width)], pool.at[half + i], gsem.at[i]
        )
        for i in range(sub)
    ]
    for one in gcopies[half:] + gcopies[:half]:
        one.start()
    wcopies = [
        pltpu.make_async_copy(w_h.at[k, :, pl.ds(off, width)], wts.at[:, pl.ds(k * width, width)], wsem.at[k])
        for k in range(slots)
    ]
    mine = pl.ds(pl.multiple_of(c * cols, cols), cols)
    theirs = pl.ds(pl.multiple_of((1 - c) * cols, cols), cols)
    near_n = pl.ds(pl.multiple_of(c * mid, mid), mid)
    far_n = pl.ds(pl.multiple_of((1 - c) * mid, mid), mid)
    edges = pl.ds(pl.multiple_of(c * mine_e, mine_e), mine_e)
    local = [
        pltpu.make_async_copy(x, y, lsem.at[i])
        for i, (x, y) in enumerate(
            [(emb_h, emb.at[c]), (win_h, win), (eo_h, eo.at[mine]), (nin_h, nin), (nout_h, nout.at[mine]),
             (src_h.at[:, edges], src), (dst_h.at[:, edges], dst)]
        )
    ]

    def remote(source, target, k, device):
        return pltpu.make_async_remote_copy(
            src_ref=source, dst_ref=target, send_sem=send.at[k], recv_sem=recv.at[k],
            device_id=device, device_id_type=MESH,
        )

    def neighbours(fwd, bwd):
        def end():
            @pl.when(has_up)
            def _():
                fwd.wait_send()
                bwd.wait_recv()

            @pl.when(has_down)
            def _():
                bwd.wait_send()
                fwd.wait_recv()

        return (lambda: pl.when(has_up)(fwd.start)), (lambda: pl.when(has_down)(bwd.start)), end

    halo_up, halo_down, halo_end = neighbours(
        remote(pool.at[pl.ds(sub, half)], pool.at[pl.ds(0, half)], 0, above),
        remote(pool.at[pl.ds(half, half)], pool.at[pl.ds(half + sub, half)], 1, below),
    )
    sent = pl.ds(0, ROWS)
    rows_up, rows_down, rows_end = neighbours(
        remote(ext.at[1, sent], ext.at[0, sent], 2, above), remote(ext.at[1, sent], ext.at[2, sent], 3, below)
    )
    weights = [
        remote(emb_h, emb.at[c], 4, partner), remote(eo_h, eo.at[mine], 5, partner),
        remote(nout_h, nout.at[mine], 6, partner),
    ]

    column = lax.broadcasted_iota(jnp.int32, (channels, width), 1) + c * width
    for one in gcopies:
        one.wait()
    for i in range(half, sub):
        block = pool[half + i]
        pool[half + i] = jnp.where(column < live[0] - i * block_len, block, jnp.zeros_like(block))
    pl.semaphore_wait(barrier, 1 + has_up.astype(jnp.int32) + has_down.astype(jnp.int32))
    halo_down()
    halo_up()
    for one in local + wcopies + weights:
        one.start()

    pool[dead] = jnp.zeros((channels, width), BF16)

    @pl.when(b == 0)
    def _():
        pool[0:half] = jnp.zeros((half, channels, width), BF16)

    @pl.when(b == n - 1)
    def _():
        pool[half + sub:dead] = jnp.zeros((half, channels, width), BF16)

    embp[...] = jnp.zeros_like(embp)
    acc[...] = jnp.zeros_like(acc)
    part[...] = jnp.zeros_like(part)
    for one in local + weights:
        one.wait()
    embp[0:channels, 0:cols] = emb[0]
    embp[0:channels, cols:hid] = emb[1]
    for i in range(2):
        mixed = mm(embp[...], win[i]) * 0.5
        mt[mine, i * PAD:(i + 1) * PAD] = mixed.T.astype(BF16)
    dmix[c] = (mm(embp[...], nin[0]) * 0.5).astype(BF16)
    pmix[c] = (mm(eo[...], nin[1]) * 0.5).astype(BF16)
    shares = [
        remote(mt.at[mine], mt.at[mine], 7, partner), remote(dmix.at[c], dmix.at[c], 8, partner),
        remote(pmix.at[c], pmix.at[c], 9, partner),
    ]
    for one in shares:
        one.start()

    def hot(i, carry):
        at = pl.ds(pl.multiple_of(i * CHUNK, CHUNK), CHUNK)
        s = src[:, at] - (b - 1) * nodes
        s = jnp.where(s < nodes, s, jnp.where(s < 2 * nodes, s + nodes, s - nodes))
        d = dst[:, at] - b * nodes
        hs[:, at] = jnp.where(lax.broadcasted_iota(jnp.int32, (3 * nodes, CHUNK), 0) == s, 1.0, 0.0).astype(BF16)
        hd[:, at] = jnp.where(lax.broadcasted_iota(jnp.int32, (nodes, CHUNK), 0) == d, 1.0, 0.0).astype(BF16)
        return carry

    lax.fori_loop(0, chunks, hot, 0)
    for one in wcopies:
        one.wait()
    for k in range(slots):
        at = slice(k * width, (k + 1) * width)
        wt[at, :] = wts[:, at].T
    for one in shares:
        one.wait()
    halo_end()

    picked = []
    for k in range(slots):
        rel = jnp.clip(ids[0, k] - b * sub + half, 0, dead - 1)
        picked.append(pool[jnp.where(k < count[0], rel, dead)])
    part[0:channels, :] = mm(jnp.concatenate(picked, axis=1), wt[...])
    swap = remote(part, other, 10, partner)
    swap.start()
    swap.wait_recv()
    own = (part[...] + other[...]).astype(BF16)
    ext[1] = own
    rows_up()
    rows_down()

    gath[PAD:, :] = mm(own, hd[...]).astype(BF16)
    gown[...] = mm(own, hs[2 * nodes:, :]).astype(BF16)
    rows = ext[1, :, near_n].astype(F32).T.astype(BF16)
    inner = [mm(rows, dmix[i]) for i in range(2)]
    first = mm(rows, embp[...]).astype(BF16)
    fin[...] = first
    swap.wait_send()
    rows_end()
    near[:, 0:nodes] = ext[0]
    near[:, nodes:] = ext[2]

    def pre_of(i):
        at = slice(i * CHUNK, (i + 1) * CHUNK)
        return mm(mt[...], gath[:, at])

    def edge_phase():
        gath[0:PAD, :] = (mm(near[...], hs[0:2 * nodes, :]) + gown[...].astype(F32)).astype(BF16)
        later = pre_of(0)
        for i in range(chunks):
            pre = later
            if i + 1 < chunks:
                later = pre_of(i + 1)
            hidden = silu_of_half(pre).astype(BF16)
            acc[...] += nt(hd[:, i * CHUNK:(i + 1) * CHUNK], hidden)

    edge_phase()

    give[...] = acc[far_n].astype(BF16)
    swap = remote(give, take, 11, partner)
    swap.start()
    swap.wait()
    total = (acc[near_n] + take[...].astype(F32)).astype(BF16)
    update = [silu_of_half(inner[i] + mm(total, pmix[i])).astype(BF16) for i in range(2)]
    update = jnp.concatenate(update, axis=1)
    fin[:, theirs] = (fin[:, theirs].astype(F32) + mm(update, nout[:, theirs])).astype(BF16)
    last = remote(fin.at[:, theirs], out.at[near_n], 12, partner)
    last.start()
    out[near_n] = (fin[:, mine].astype(F32) + mm(update, nout[:, mine])).astype(BF16)
    last.wait()


def on_device(
    grid_field, band_points, block_ids, block_count, block_weight, embed_weight,
    edge_src, edge_dst, edge_in_weight, edge_out_weight, node_in_weight, node_out_weight,
):
    n = lax.axis_size("band")
    channels, points = grid_field.shape
    slots, nodes, block_len = block_weight.shape[1:]
    sub = points // block_len
    width = block_len // 2
    cols = embed_weight.shape[1]
    hid = 2 * cols
    edges = edge_src.shape[0] // 2
    bf = lambda *shape: pltpu.VMEM(shape, BF16)
    f32 = lambda *shape: pltpu.VMEM(shape, F32)
    return pl.pallas_call(
        functools.partial(layer_kernel, n),
        out_shape=jax.ShapeDtypeStruct((nodes, cols), BF16),
        in_specs=[SMEM] * 3 + [HBM] * 9, out_specs=VMEM,
        scratch_shapes=[
            bf(2 * sub + 1, channels, width), bf(nodes, slots * width), bf(slots * width, nodes),
            bf(2, channels, cols), bf(PAD, hid), bf(hid, hid), bf(2, hid, cols), bf(2, hid, cols), bf(hid, hid),
            pltpu.VMEM((1, edges), jnp.int32), pltpu.VMEM((1, edges), jnp.int32),
            bf(hid, 2 * PAD), bf(2, PAD, cols), bf(2, hid, cols), bf(3 * nodes, edges), bf(nodes, edges),
            f32(PAD, nodes), f32(PAD, nodes), bf(3, PAD, nodes), bf(PAD, 2 * nodes),
            bf(PAD, edges), bf(2 * PAD, edges), f32(nodes, hid),
            bf(nodes // 2, hid), bf(nodes // 2, hid), bf(nodes // 2, hid),
            pltpu.SemaphoreType.DMA((slots,)), pltpu.SemaphoreType.DMA((sub,)), pltpu.SemaphoreType.DMA((7,)),
            pltpu.SemaphoreType.DMA((13,)), pltpu.SemaphoreType.DMA((13,)),
        ],
        compiler_params=pltpu.CompilerParams(vmem_limit_bytes=LARGE, collective_id=0, has_side_effects=True),
    )(
        block_ids, block_count, band_points, grid_field, block_weight.reshape(block_weight.shape[1:]),
        embed_weight, edge_out_weight, edge_in_weight, node_in_weight, node_out_weight,
        edge_src.reshape(1, -1), edge_dst.reshape(1, -1),
    )


def solution(mesh):
    return jax.shard_map(
        on_device,
        mesh=mesh,
        in_specs=(
            P(None, "band"), P("band"), P("band", None), P("band"),
            P("band", None, None, None), P(None, "ch"), P("band"), P("band"),
            P(None, None, "ch"), P("ch", None), P(None, None, "ch"), P("ch", None),
        ),
        out_specs=P("band", "ch"),
        check_vma=False,
    )
```

```python
import functools

import jax
import jax.numpy as jnp
from jax import lax
from jax.experimental import pallas as pl
from jax.experimental.pallas import tpu as pltpu
from jax.sharding import PartitionSpec as P

MESH = pl.DeviceIdType.MESH
F32 = jnp.float32
BF16 = jnp.bfloat16
VMEM = pl.BlockSpec(memory_space=pltpu.VMEM)
SMEM = pl.BlockSpec(memory_space=pltpu.SMEM)
HBM = pl.BlockSpec(memory_space=pltpu.HBM)
LARGE = int(50 * 1024 * 1024)
CHUNK = 512
PAD = 128
ROWS = 112


def nt(x, y):
    return lax.dot_general(x, y, (((1,), (1,)), ((), ())), preferred_element_type=F32)


def mm(x, y):
    return jnp.dot(x, y, preferred_element_type=F32)


def silu_of_half(v):
    return v + v * jnp.tanh(v)


def layer_kernel(
    n, count, live, ids_h, grid_h, w_h, emb_h, eo_h, win_h, nin_h, nout_h, src_h, dst_h, out,
    ids, pool, wts, wt, emb, embp, eo, win, nin, nout, src, dst,
    mt, mix, hs, hd, part, other, ext, near, gown, gath, acc, give, take, fin,
    ssem, wsem, gsem, lsem, send, recv,
):
    b = lax.axis_index("band")
    c = lax.axis_index("ch")
    slots, nodes, block_len = w_h.shape
    width = block_len // 2
    channels = grid_h.shape[0]
    sub = grid_h.shape[1] // block_len
    half = sub // 2
    cols = emb_h.shape[1]
    hid = 2 * cols
    mine_e = src.shape[1]
    chunks = mine_e // CHUNK
    mid = nodes // 2
    dead = 2 * sub
    up, down = jnp.minimum(b + 1, n - 1), jnp.maximum(b - 1, 0)
    has_up, has_down = b < n - 1, b > 0
    above, below, partner = (up, c), (down, c), (b, 1 - c)

    ext[...] = jnp.zeros_like(ext)
    barrier = pltpu.get_barrier_semaphore()

    @pl.when(has_up)
    def _():
        pl.semaphore_signal(barrier, inc=1, device_id=above, device_id_type=MESH)

    @pl.when(has_down)
    def _():
        pl.semaphore_signal(barrier, inc=1, device_id=below, device_id_type=MESH)

    pl.semaphore_signal(barrier, inc=1, device_id=partner, device_id_type=MESH)

    off = pl.multiple_of(c * width, width)
    gcopies = [
        pltpu.make_async_copy(
            grid_h.at[:, pl.ds(pl.multiple_of((2 * i + c) * width, width), width)], pool.at[half + i], gsem
        )
        for i in range(sub)
    ]
    names = pltpu.make_async_copy(ids_h, ids, ssem)
    for one in [names] + gcopies[half:] + gcopies[:half]:
        one.start()
    wcopy = pltpu.make_async_copy(w_h.at[:, :, pl.ds(off, width)], wts, wsem)
    mine = pl.ds(pl.multiple_of(c * cols, cols), cols)
    theirs = pl.ds(pl.multiple_of((1 - c) * cols, cols), cols)
    near_n = pl.ds(pl.multiple_of(c * mid, mid), mid)
    far_n = pl.ds(pl.multiple_of((1 - c) * mid, mid), mid)
    edges = pl.ds(pl.multiple_of(c * mine_e, mine_e), mine_e)
    local = [
        pltpu.make_async_copy(x, y, lsem.at[i])
        for i, (x, y) in enumerate(
            [(emb_h, emb.at[c]), (win_h, win), (eo_h, eo.at[mine]), (nin_h, nin), (nout_h, nout.at[mine]),
             (src_h.at[:, edges], src), (dst_h.at[:, edges], dst)]
        )
    ]

    def remote(source, target, k, device):
        return pltpu.make_async_remote_copy(
            src_ref=source, dst_ref=target, send_sem=send.at[k], recv_sem=recv.at[k],
            device_id=device, device_id_type=MESH,
        )

    def neighbours(fwd, bwd):
        def end():
            @pl.when(has_up)
            def _():
                fwd.wait_send()
                bwd.wait_recv()

            @pl.when(has_down)
            def _():
                bwd.wait_send()
                fwd.wait_recv()

        return (lambda: pl.when(has_up)(fwd.start)), (lambda: pl.when(has_down)(bwd.start)), end

    halo_up, halo_down, halo_end = neighbours(
        remote(pool.at[pl.ds(sub, half)], pool.at[pl.ds(0, half)], 0, above),
        remote(pool.at[pl.ds(half, half)], pool.at[pl.ds(half + sub, half)], 1, below),
    )
    sent = pl.ds(0, ROWS)
    rows_up, rows_down, rows_end = neighbours(
        remote(ext.at[1, sent], ext.at[0, sent], 2, above), remote(ext.at[1, sent], ext.at[2, sent], 3, below)
    )
    weights = [
        remote(emb_h, emb.at[c], 4, partner), remote(eo_h, eo.at[mine], 5, partner),
        remote(nout_h, nout.at[mine], 6, partner),
    ]

    column = lax.broadcasted_iota(jnp.int32, (channels, width), 1) + c * width
    pltpu.make_async_copy(pool.at[pl.ds(half, sub)], pool.at[pl.ds(half, sub)], gsem).wait()
    names.wait()
    for i in range(half, sub):
        block = pool[half + i]
        pool[half + i] = jnp.where(column < live[0] - i * block_len, block, jnp.zeros_like(block))
    pl.semaphore_wait(barrier, 1 + has_up.astype(jnp.int32) + has_down.astype(jnp.int32))
    halo_down()
    halo_up()
    for one in local + [wcopy] + weights:
        one.start()

    pool[dead] = jnp.zeros((channels, width), BF16)

    @pl.when(b == 0)
    def _():
        pool[0:half] = jnp.zeros((half, channels, width), BF16)

    @pl.when(b == n - 1)
    def _():
        pool[half + sub:dead] = jnp.zeros((half, channels, width), BF16)

    embp[...] = jnp.zeros_like(embp)
    acc[...] = jnp.zeros_like(acc)
    part[...] = jnp.zeros_like(part)
    for one in local + weights:
        one.wait()
    embp[0:channels, 0:cols] = emb[0]
    embp[0:channels, cols:hid] = emb[1]
    for i in range(2):
        mixed = mm(embp[...], win[i]) * 0.5
        mt[mine, i * PAD:(i + 1) * PAD] = mixed.T.astype(BF16)
    mix[c, hid:] = (mm(embp[...], nin[0]) * 0.5).astype(BF16)
    mix[c, 0:hid] = (mm(eo[...], nin[1]) * 0.5).astype(BF16)
    shares = [
        remote(mt.at[mine], mt.at[mine], 7, partner), remote(mix.at[c], mix.at[c], 8, partner),
    ]
    for one in shares:
        one.start()

    def hot(i, carry):
        at = pl.ds(pl.multiple_of(i * CHUNK, CHUNK), CHUNK)
        s = src[:, at] - (b - 1) * nodes
        s = jnp.where(s < nodes, s, jnp.where(s < 2 * nodes, s + nodes, s - nodes))
        d = dst[:, at] - b * nodes
        hs[:, at] = jnp.where(lax.broadcasted_iota(jnp.int32, (3 * nodes, CHUNK), 0) == s, 1.0, 0.0).astype(BF16)
        hd[:, at] = jnp.where(lax.broadcasted_iota(jnp.int32, (nodes, CHUNK), 0) == d, 1.0, 0.0).astype(BF16)
        return carry

    lax.fori_loop(0, chunks, hot, 0)
    wcopy.wait()
    for k in range(slots):
        wt[k * width:(k + 1) * width, :] = wts[k].T
    for one in shares:
        one.wait()
    halo_end()

    picked = []
    for k in range(slots):
        rel = jnp.clip(ids[0, k] - b * sub + half, 0, dead - 1)
        picked.append(pool[jnp.where(k < count[0], rel, dead)])
    part[0:channels, :] = mm(jnp.concatenate(picked, axis=1), wt[...])
    swap = remote(part, other, 9, partner)
    swap.start()
    swap.wait_recv()
    own = (part[...] + other[...]).astype(BF16)
    ext[1] = own
    rows_up()
    rows_down()

    gath[PAD:, :] = mm(own, hd[...]).astype(BF16)
    gown[...] = mm(own, hs[2 * nodes:, :]).astype(BF16)
    rows = ext[1, :, near_n].astype(F32).T.astype(BF16)
    inner = [mm(rows, mix[i, hid:]) for i in range(2)]
    first = mm(rows, embp[...]).astype(BF16)
    fin[...] = first
    swap.wait_send()
    rows_end()
    near[:, 0:nodes] = ext[0]
    near[:, nodes:] = ext[2]

    def pre_of(i):
        at = slice(i * CHUNK, (i + 1) * CHUNK)
        return mm(mt[...], gath[:, at])

    def edge_phase():
        gath[0:PAD, :] = (mm(near[...], hs[0:2 * nodes, :]) + gown[...].astype(F32)).astype(BF16)
        later = pre_of(0)
        for i in range(chunks):
            pre = later
            if i + 1 < chunks:
                later = pre_of(i + 1)
            hidden = silu_of_half(pre).astype(BF16)
            acc[...] += nt(hd[:, i * CHUNK:(i + 1) * CHUNK], hidden)

    edge_phase()

    give[...] = acc[far_n].astype(BF16)
    swap = remote(give, take, 10, partner)
    swap.start()
    swap.wait()
    total = (acc[near_n] + take[...].astype(F32)).astype(BF16)
    update = [silu_of_half(inner[i] + mm(total, mix[i, 0:hid])).astype(BF16) for i in range(2)]
    update = jnp.concatenate(update, axis=1)
    fin[:, theirs] = (fin[:, theirs].astype(F32) + mm(update, nout[:, theirs])).astype(BF16)
    last = remote(fin.at[:, theirs], out.at[near_n], 11, partner)
    last.start()
    out[near_n] = (fin[:, mine].astype(F32) + mm(update, nout[:, mine])).astype(BF16)
    last.wait()


def on_device(
    grid_field, band_points, block_ids, block_count, block_weight, embed_weight,
    edge_src, edge_dst, edge_in_weight, edge_out_weight, node_in_weight, node_out_weight,
):
    n = lax.axis_size("band")
    channels, points = grid_field.shape
    slots, nodes, block_len = block_weight.shape[1:]
    sub = points // block_len
    width = block_len // 2
    cols = embed_weight.shape[1]
    hid = 2 * cols
    edges = edge_src.shape[0] // 2
    bf = lambda *shape: pltpu.VMEM(shape, BF16)
    f32 = lambda *shape: pltpu.VMEM(shape, F32)
    return pl.pallas_call(
        functools.partial(layer_kernel, n),
        out_shape=pltpu.VMEM((nodes, cols), BF16),
        in_specs=[SMEM] * 2 + [HBM] * 10, out_specs=VMEM,
        scratch_shapes=[
            pltpu.SMEM((1, slots), jnp.int32),
            bf(2 * sub + 1, channels, width), bf(slots, nodes, width), bf(slots * width, nodes),
            bf(2, channels, cols), bf(PAD, hid), bf(hid, hid), bf(2, hid, cols), bf(2, hid, cols), bf(hid, hid),
            pltpu.VMEM((1, edges), jnp.int32), pltpu.VMEM((1, edges), jnp.int32),
            bf(hid, 2 * PAD), bf(2, hid + PAD, cols), bf(3 * nodes, edges), bf(nodes, edges),
            f32(PAD, nodes), f32(PAD, nodes), bf(3, PAD, nodes), bf(PAD, 2 * nodes),
            bf(PAD, edges), bf(2 * PAD, edges), f32(nodes, hid),
            bf(nodes // 2, hid), bf(nodes // 2, hid), bf(nodes // 2, hid),
            pltpu.SemaphoreType.DMA, pltpu.SemaphoreType.DMA, pltpu.SemaphoreType.DMA, pltpu.SemaphoreType.DMA((7,)),
            pltpu.SemaphoreType.DMA((12,)), pltpu.SemaphoreType.DMA((12,)),
        ],
        compiler_params=pltpu.CompilerParams(vmem_limit_bytes=LARGE, collective_id=0, has_side_effects=True),
    )(
        block_count, band_points, *[pltpu.with_memory_space_constraint(x, pltpu.HBM) for x in (
            block_ids, grid_field, block_weight.reshape(block_weight.shape[1:]),
            embed_weight, edge_out_weight, edge_in_weight, node_in_weight, node_out_weight,
            edge_src.reshape(1, -1), edge_dst.reshape(1, -1),
        )],
    )


def solution(mesh):
    return jax.shard_map(
        on_device,
        mesh=mesh,
        in_specs=(
            P(None, "band"), P("band"), P("band", None), P("band"),
            P("band", None, None, None), P(None, "ch"), P("band"), P("band"),
            P(None, None, "ch"), P("ch", None), P(None, None, "ch"), P("ch", None),
        ),
        out_specs=P("band", "ch"),
        check_vma=False,
    )
```

```python
import functools

import jax
import jax.numpy as jnp
from jax import lax
from jax.experimental import pallas as pl
from jax.experimental.pallas import tpu as pltpu
from jax.sharding import PartitionSpec as P

MESH = pl.DeviceIdType.MESH
F32 = jnp.float32
BF16 = jnp.bfloat16
VMEM = pl.BlockSpec(memory_space=pltpu.VMEM)
SMEM = pl.BlockSpec(memory_space=pltpu.SMEM)
HBM = pl.BlockSpec(memory_space=pltpu.HBM)
LARGE = int(50 * 1024 * 1024)
CHUNK = 512
PAD = 128
ROWS = 112
TILE = 16


def nt(x, y):
    return lax.dot_general(x, y, (((1,), (1,)), ((), ())), preferred_element_type=F32)


def mm(x, y):
    return jnp.dot(x, y, preferred_element_type=F32)


def silu_of_half(v):
    return v + v * jnp.tanh(v)


def layer_kernel(
    n, count, live, ids_h, grid_h, w_h, emb_h, eo_h, win_h, nin_h, nout_h, src_h, dst_h, out,
    ids, raw, pool, wts, wt, emb, embp, eo, win, nin, nout, src, dst,
    mt, mix, hs, hd, part, other, ext, near, gown, gath, acc, give, take, fin,
    ssem, wsem, gsem, lsem, send, recv,
):
    b = lax.axis_index("band")
    c = lax.axis_index("ch")
    slots, nodes, block_len = w_h.shape
    width = block_len // 2
    channels = grid_h.shape[0]
    sub = grid_h.shape[1] // block_len
    half = sub // 2
    cols = emb_h.shape[1]
    hid = 2 * cols
    mine_e = src.shape[1]
    chunks = mine_e // CHUNK
    mid = nodes // 2
    tall = channels // TILE
    tail = channels % TILE
    group = TILE // tail
    quarter = (tall * half) + half // group
    up, down = jnp.minimum(b + 1, n - 1), jnp.maximum(b - 1, 0)
    has_up, has_down = b < n - 1, b > 0
    above, below, partner = (up, c), (down, c), (b, 1 - c)

    ext[...] = jnp.zeros_like(ext)
    barrier = pltpu.get_barrier_semaphore()

    @pl.when(has_up)
    def _():
        pl.semaphore_signal(barrier, inc=1, device_id=above, device_id_type=MESH)

    @pl.when(has_down)
    def _():
        pl.semaphore_signal(barrier, inc=1, device_id=below, device_id_type=MESH)

    pl.semaphore_signal(barrier, inc=1, device_id=partner, device_id_type=MESH)

    off = pl.multiple_of(c * width, width)
    gcopies = [
        pltpu.make_async_copy(
            grid_h.at[:, pl.ds(pl.multiple_of((2 * i + c) * width, width), width)], raw.at[i], gsem
        )
        for i in range(sub)
    ]
    names = pltpu.make_async_copy(ids_h, ids, ssem)
    for one in [names] + gcopies[half:] + gcopies[:half]:
        one.start()
    wcopy = pltpu.make_async_copy(w_h.at[:, :, pl.ds(off, width)], wts, wsem)
    mine = pl.ds(pl.multiple_of(c * cols, cols), cols)
    theirs = pl.ds(pl.multiple_of((1 - c) * cols, cols), cols)
    near_n = pl.ds(pl.multiple_of(c * mid, mid), mid)
    far_n = pl.ds(pl.multiple_of((1 - c) * mid, mid), mid)
    edges = pl.ds(pl.multiple_of(c * mine_e, mine_e), mine_e)
    local = [
        pltpu.make_async_copy(x, y, lsem.at[i])
        for i, (x, y) in enumerate(
            [(emb_h, emb.at[c]), (win_h, win), (eo_h, eo.at[mine]), (nin_h, nin), (nout_h, nout.at[mine]),
             (src_h.at[:, edges], src), (dst_h.at[:, edges], dst)]
        )
    ]

    def remote(source, target, k, device):
        return pltpu.make_async_remote_copy(
            src_ref=source, dst_ref=target, send_sem=send.at[k], recv_sem=recv.at[k],
            device_id=device, device_id_type=MESH,
        )

    def neighbours(fwd, bwd):
        def end():
            @pl.when(has_up)
            def _():
                fwd.wait_send()
                bwd.wait_recv()

            @pl.when(has_down)
            def _():
                bwd.wait_send()
                fwd.wait_recv()

        return (lambda: pl.when(has_up)(fwd.start)), (lambda: pl.when(has_down)(bwd.start)), end

    halo_up, halo_down, halo_end = neighbours(
        remote(pool.at[pl.ds(2 * quarter, quarter)], pool.at[pl.ds(0, quarter)], 0, above),
        remote(pool.at[pl.ds(quarter, quarter)], pool.at[pl.ds(3 * quarter, quarter)], 1, below),
    )
    sent = pl.ds(0, ROWS)
    rows_up, rows_down, rows_end = neighbours(
        remote(ext.at[1, sent], ext.at[0, sent], 2, above), remote(ext.at[1, sent], ext.at[2, sent], 3, below)
    )
    weights = [
        remote(emb_h, emb.at[c], 4, partner), remote(eo_h, eo.at[mine], 5, partner),
        remote(nout_h, nout.at[mine], 6, partner),
    ]

    column = lax.broadcasted_iota(jnp.int32, (channels, width), 1) + c * width
    pltpu.make_async_copy(raw, raw, gsem).wait()
    names.wait()
    for i in range(0, sub, group):
        ends = []
        base, first_of = (1 + i // half) * quarter, i % half
        for j in range(group):
            block = raw[i + j]
            if i >= half:
                block = jnp.where(column < live[0] - (i + j) * block_len, block, jnp.zeros_like(block))
            for t in range(tall):
                pool[base + (first_of + j) * tall + t] = block[t * TILE:(t + 1) * TILE]
            ends.append(block[tall * TILE:].astype(F32))
        pool[base + tall * half + first_of // group] = jnp.concatenate(ends, axis=0).astype(BF16)
    pl.semaphore_wait(barrier, 1 + has_up.astype(jnp.int32) + has_down.astype(jnp.int32))
    halo_down()
    halo_up()
    for one in local + [wcopy] + weights:
        one.start()

    blank = jnp.zeros((quarter,) + pool.shape[1:], BF16)
    pool[4 * quarter:] = blank

    @pl.when(b == 0)
    def _():
        pool[0:quarter] = blank

    @pl.when(b == n - 1)
    def _():
        pool[3 * quarter:4 * quarter] = blank

    embp[...] = jnp.zeros_like(embp)
    acc[...] = jnp.zeros_like(acc)
    part[...] = jnp.zeros_like(part)
    for one in local + weights:
        one.wait()
    embp[0:channels, 0:cols] = emb[0]
    embp[0:channels, cols:hid] = emb[1]
    for i in range(2):
        mixed = mm(embp[...], win[i]) * 0.5
        mt[mine, i * PAD:(i + 1) * PAD] = mixed.T.astype(BF16)
    mix[c, hid:] = (mm(embp[...], nin[0]) * 0.5).astype(BF16)
    mix[c, 0:hid] = (mm(eo[...], nin[1]) * 0.5).astype(BF16)
    shares = [
        remote(mt.at[mine], mt.at[mine], 7, partner), remote(mix.at[c], mix.at[c], 8, partner),
    ]
    for one in shares:
        one.start()

    def hot(i, carry):
        at = pl.ds(pl.multiple_of(i * CHUNK, CHUNK), CHUNK)
        s = src[:, at] - (b - 1) * nodes
        s = jnp.where(s < nodes, s, jnp.where(s < 2 * nodes, s + nodes, s - nodes))
        d = dst[:, at] - b * nodes
        hs[:, at] = jnp.where(lax.broadcasted_iota(jnp.int32, (3 * nodes, CHUNK), 0) == s, 1.0, 0.0).astype(BF16)
        hd[:, at] = jnp.where(lax.broadcasted_iota(jnp.int32, (nodes, CHUNK), 0) == d, 1.0, 0.0).astype(BF16)
        return carry

    lax.fori_loop(0, chunks, hot, 0)
    wcopy.wait()
    for k in range(slots):
        wt[k * width:(k + 1) * width, :] = wts[k].T
    for one in shares:
        one.wait()
    halo_end()

    picked = []
    line = lax.broadcasted_iota(jnp.int32, (TILE, width), 0)
    for k in range(slots):
        rel = jnp.clip(ids[0, k] - b * sub + half, 0, 2 * sub - 1)
        part_of, i = rel // half, rel % half
        base = jnp.where(k < count[0], part_of, 4) * quarter
        low = i % group * tail
        ends = pool[base + tall * half + i // group]
        ends = jnp.where((line >= low) & (line < low + tail), ends, jnp.zeros_like(ends))
        tiles = [pool[base + i * tall + t] for t in range(tall)]
        picked.append(jnp.concatenate(tiles + [ends], axis=0))
    mixed = mm(jnp.concatenate(picked, axis=1), wt[...])
    top = tall * TILE
    part[0:top, :] = mixed[:top]
    part[top:channels, :] = sum(mixed[top + j * tail:top + (j + 1) * tail] for j in range(group))
    swap = remote(part, other, 9, partner)
    swap.start()
    swap.wait_recv()
    own = (part[...] + other[...]).astype(BF16)
    ext[1] = own
    rows_up()
    rows_down()

    gath[PAD:, :] = mm(own, hd[...]).astype(BF16)
    gown[...] = mm(own, hs[2 * nodes:, :]).astype(BF16)
    rows = ext[1, :, near_n].astype(F32).T.astype(BF16)
    inner = [mm(rows, mix[i, hid:]) for i in range(2)]
    first = mm(rows, embp[...]).astype(BF16)
    fin[...] = first
    swap.wait_send()
    rows_end()
    near[:, 0:nodes] = ext[0]
    near[:, nodes:] = ext[2]

    def pre_of(i):
        at = slice(i * CHUNK, (i + 1) * CHUNK)
        return mm(mt[...], gath[:, at])

    def edge_phase():
        gath[0:PAD, :] = (mm(near[...], hs[0:2 * nodes, :]) + gown[...].astype(F32)).astype(BF16)
        later = pre_of(0)
        for i in range(chunks):
            pre = later
            if i + 1 < chunks:
                later = pre_of(i + 1)
            hidden = silu_of_half(pre).astype(BF16)
            acc[...] += nt(hd[:, i * CHUNK:(i + 1) * CHUNK], hidden)

    edge_phase()

    give[...] = acc[far_n].astype(BF16)
    swap = remote(give, take, 10, partner)
    swap.start()
    swap.wait()
    total = (acc[near_n] + take[...].astype(F32)).astype(BF16)
    update = [silu_of_half(inner[i] + mm(total, mix[i, 0:hid])).astype(BF16) for i in range(2)]
    update = jnp.concatenate(update, axis=1)
    fin[:, theirs] = (fin[:, theirs].astype(F32) + mm(update, nout[:, theirs])).astype(BF16)
    last = remote(fin.at[:, theirs], out.at[near_n], 11, partner)
    last.start()
    out[near_n] = (fin[:, mine].astype(F32) + mm(update, nout[:, mine])).astype(BF16)
    last.wait()


def on_device(
    grid_field, band_points, block_ids, block_count, block_weight, embed_weight,
    edge_src, edge_dst, edge_in_weight, edge_out_weight, node_in_weight, node_out_weight,
):
    n = lax.axis_size("band")
    channels, points = grid_field.shape
    slots, nodes, block_len = block_weight.shape[1:]
    sub = points // block_len
    width = block_len // 2
    cols = embed_weight.shape[1]
    hid = 2 * cols
    edges = edge_src.shape[0] // 2
    bf = lambda *shape: pltpu.VMEM(shape, BF16)
    f32 = lambda *shape: pltpu.VMEM(shape, F32)
    return pl.pallas_call(
        functools.partial(layer_kernel, n),
        out_shape=pltpu.VMEM((nodes, cols), BF16),
        in_specs=[SMEM] * 2 + [HBM] * 10, out_specs=VMEM,
        scratch_shapes=[
            pltpu.SMEM((1, slots), jnp.int32),
            bf(sub, channels, width), bf(5 * channels * sub // 2 // TILE, TILE, width), bf(slots, nodes, width), bf(slots * width, nodes),
            bf(2, channels, cols), bf(PAD, hid), bf(hid, hid), bf(2, hid, cols), bf(2, hid, cols), bf(hid, hid),
            pltpu.VMEM((1, edges), jnp.int32), pltpu.VMEM((1, edges), jnp.int32),
            bf(hid, 2 * PAD), bf(2, hid + PAD, cols), bf(3 * nodes, edges), bf(nodes, edges),
            f32(PAD, nodes), f32(PAD, nodes), bf(3, PAD, nodes), bf(PAD, 2 * nodes),
            bf(PAD, edges), bf(2 * PAD, edges), f32(nodes, hid),
            bf(nodes // 2, hid), bf(nodes // 2, hid), bf(nodes // 2, hid),
            pltpu.SemaphoreType.DMA, pltpu.SemaphoreType.DMA, pltpu.SemaphoreType.DMA, pltpu.SemaphoreType.DMA((7,)),
            pltpu.SemaphoreType.DMA((12,)), pltpu.SemaphoreType.DMA((12,)),
        ],
        compiler_params=pltpu.CompilerParams(vmem_limit_bytes=LARGE, collective_id=0, has_side_effects=True),
    )(
        block_count, band_points, *[pltpu.with_memory_space_constraint(x, pltpu.HBM) for x in (
            block_ids, grid_field, block_weight.reshape(block_weight.shape[1:]),
            embed_weight, edge_out_weight, edge_in_weight, node_in_weight, node_out_weight,
            edge_src.reshape(1, -1), edge_dst.reshape(1, -1),
        )],
    )


def solution(mesh):
    return jax.shard_map(
        on_device,
        mesh=mesh,
        in_specs=(
            P(None, "band"), P("band"), P("band", None), P("band"),
            P("band", None, None, None), P(None, "ch"), P("band"), P("band"),
            P(None, None, "ch"), P("ch", None), P(None, None, "ch"), P("ch", None),
        ),
        out_specs=P("band", "ch"),
        check_vma=False,
    )
```

```python
import functools

import jax
import jax.numpy as jnp
from jax import lax
from jax.experimental import pallas as pl
from jax.experimental.pallas import tpu as pltpu
from jax.sharding import PartitionSpec as P

MESH = pl.DeviceIdType.MESH
F32 = jnp.float32
BF16 = jnp.bfloat16
VMEM = pl.BlockSpec(memory_space=pltpu.VMEM)
SMEM = pl.BlockSpec(memory_space=pltpu.SMEM)
HBM = pl.BlockSpec(memory_space=pltpu.HBM)
LARGE = int(50 * 1024 * 1024)
CHUNK = 512
PAD = 128
ROWS = 112
TILE = 16


def nt(x, y):
    return lax.dot_general(x, y, (((1,), (1,)), ((), ())), preferred_element_type=F32)


def mm(x, y):
    return jnp.dot(x, y, preferred_element_type=F32)


def silu_of_half(v):
    return v + v * jnp.tanh(v)


def layer_kernel(
    n, count, live, ids_h, grid_h, w_h, emb_h, eo_h, win_h, nin_h, nout_h, src_h, dst_h, out,
    ids, raw, pool, wts, wt, emb, embp, eo, win, nin, nout, src, dst,
    mt, mix, hs, hd, part, other, ext, gown, gath, acc, give, take, fin,
    ssem, wsem, gsem, lsem, send, recv,
):
    b = lax.axis_index("band")
    c = lax.axis_index("ch")
    slots, nodes, block_len = w_h.shape
    width = block_len // 2
    channels = grid_h.shape[0]
    sub = grid_h.shape[1] // block_len
    half = sub // 2
    cols = emb_h.shape[1]
    hid = 2 * cols
    mine_e = src.shape[1]
    chunks = mine_e // CHUNK
    mid = nodes // 2
    tall = channels // TILE
    tail = channels % TILE
    group = TILE // tail
    quarter = (tall * half) + half // group
    up, down = jnp.minimum(b + 1, n - 1), jnp.maximum(b - 1, 0)
    has_up, has_down = b < n - 1, b > 0
    above, below, partner = (up, c), (down, c), (b, 1 - c)

    ext[...] = jnp.zeros_like(ext)
    barrier = pltpu.get_barrier_semaphore()

    @pl.when(has_up)
    def _():
        pl.semaphore_signal(barrier, inc=1, device_id=above, device_id_type=MESH)

    @pl.when(has_down)
    def _():
        pl.semaphore_signal(barrier, inc=1, device_id=below, device_id_type=MESH)

    pl.semaphore_signal(barrier, inc=1, device_id=partner, device_id_type=MESH)

    off = pl.multiple_of(c * width, width)
    gcopies = [
        pltpu.make_async_copy(
            grid_h.at[:, pl.ds(pl.multiple_of((2 * i + c) * width, width), width)], raw.at[i], gsem
        )
        for i in range(sub)
    ]
    names = pltpu.make_async_copy(ids_h, ids, ssem)
    for one in [names] + gcopies[half:] + gcopies[:half]:
        one.start()
    wcopy = pltpu.make_async_copy(w_h.at[:, :, pl.ds(off, width)], wts, wsem)
    mine = pl.ds(pl.multiple_of(c * cols, cols), cols)
    theirs = pl.ds(pl.multiple_of((1 - c) * cols, cols), cols)
    near_n = pl.ds(pl.multiple_of(c * mid, mid), mid)
    far_n = pl.ds(pl.multiple_of((1 - c) * mid, mid), mid)
    edges = pl.ds(pl.multiple_of(c * mine_e, mine_e), mine_e)
    local = [
        pltpu.make_async_copy(x, y, lsem.at[i])
        for i, (x, y) in enumerate(
            [(emb_h, emb.at[c]), (win_h, win), (eo_h, eo.at[mine]), (nin_h, nin), (nout_h, nout.at[mine]),
             (src_h.at[:, edges], src), (dst_h.at[:, edges], dst)]
        )
    ]

    def remote(source, target, k, device):
        return pltpu.make_async_remote_copy(
            src_ref=source, dst_ref=target, send_sem=send.at[k], recv_sem=recv.at[k],
            device_id=device, device_id_type=MESH,
        )

    def neighbours(fwd, bwd):
        def end_up():
            @pl.when(has_up)
            def _():
                fwd.wait_send()
                bwd.wait_recv()

        def end_down():
            @pl.when(has_down)
            def _():
                bwd.wait_send()
                fwd.wait_recv()

        return (lambda: pl.when(has_up)(fwd.start)), (lambda: pl.when(has_down)(bwd.start)), end_up, end_down

    halo_up, halo_down, halo_end_up, halo_end_down = neighbours(
        remote(pool.at[pl.ds(2 * quarter, quarter)], pool.at[pl.ds(0, quarter)], 0, above),
        remote(pool.at[pl.ds(quarter, quarter)], pool.at[pl.ds(3 * quarter, quarter)], 1, below),
    )
    sent = pl.ds(0, ROWS)
    rows_up, rows_down, rows_end_up, rows_end_down = neighbours(
        remote(ext.at[1, sent], ext.at[0, sent], 2, above), remote(ext.at[1, sent], ext.at[2, sent], 3, below)
    )
    weights = [
        remote(emb_h, emb.at[c], 4, partner), remote(eo_h, eo.at[mine], 5, partner),
        remote(nout_h, nout.at[mine], 6, partner),
    ]

    column = lax.broadcasted_iota(jnp.int32, (channels, width), 1) + c * width
    pltpu.make_async_copy(raw, raw, gsem).wait()
    names.wait()
    for i in range(0, sub, group):
        ends = []
        base, first_of = (1 + i // half) * quarter, i % half
        for j in range(group):
            block = raw[i + j]
            if i >= half:
                block = jnp.where(column < live[0] - (i + j) * block_len, block, jnp.zeros_like(block))
            for t in range(tall):
                pool[base + (first_of + j) * tall + t] = block[t * TILE:(t + 1) * TILE]
            ends.append(block[tall * TILE:].astype(F32))
        pool[base + tall * half + first_of // group] = jnp.concatenate(ends, axis=0).astype(BF16)
    pl.semaphore_wait(barrier, 1 + has_up.astype(jnp.int32) + has_down.astype(jnp.int32))
    halo_down()
    halo_up()
    for one in local + [wcopy] + weights:
        one.start()

    blank = jnp.zeros((quarter,) + pool.shape[1:], BF16)
    pool[4 * quarter:] = blank

    @pl.when(b == 0)
    def _():
        pool[0:quarter] = blank

    @pl.when(b == n - 1)
    def _():
        pool[3 * quarter:4 * quarter] = blank

    embp[...] = jnp.zeros_like(embp)
    acc[...] = jnp.zeros_like(acc)
    part[...] = jnp.zeros_like(part)
    for one in local + weights:
        one.wait()
    embp[0:channels, 0:cols] = emb[0]
    embp[0:channels, cols:hid] = emb[1]
    for i in range(2):
        mixed = mm(embp[...], win[i]) * 0.5
        mt[mine, i * PAD:(i + 1) * PAD] = mixed.T.astype(BF16)
    mix[c, hid:] = (mm(embp[...], nin[0]) * 0.5).astype(BF16)
    mix[c, 0:hid] = (mm(eo[...], nin[1]) * 0.5).astype(BF16)
    shares = [
        remote(mt.at[mine], mt.at[mine], 7, partner), remote(mix.at[c], mix.at[c], 8, partner),
    ]
    for one in shares:
        one.start()

    def hot(i, carry):
        at = pl.ds(pl.multiple_of(i * CHUNK, CHUNK), CHUNK)
        s = src[:, at] - (b - 1) * nodes
        s = jnp.where(s < nodes, s, jnp.where(s < 2 * nodes, s + nodes, s - nodes))
        d = dst[:, at] - b * nodes
        hs[:, at] = jnp.where(lax.broadcasted_iota(jnp.int32, (3 * nodes, CHUNK), 0) == s, 1.0, 0.0).astype(BF16)
        hd[:, at] = jnp.where(lax.broadcasted_iota(jnp.int32, (nodes, CHUNK), 0) == d, 1.0, 0.0).astype(BF16)
        return carry

    lax.fori_loop(0, chunks, hot, 0)
    wcopy.wait()
    for k in range(slots):
        wt[k * width:(k + 1) * width, :] = wts[k].T
    for one in shares:
        one.wait()
    halo_end_up()
    halo_end_down()

    picked = []
    line = lax.broadcasted_iota(jnp.int32, (TILE, width), 0)
    for k in range(slots):
        rel = jnp.clip(ids[0, k] - b * sub + half, 0, 2 * sub - 1)
        part_of, i = rel // half, rel % half
        base = jnp.where(k < count[0], part_of, 4) * quarter
        low = i % group * tail
        ends = pool[base + tall * half + i // group]
        ends = jnp.where((line >= low) & (line < low + tail), ends, jnp.zeros_like(ends))
        tiles = [pool[base + i * tall + t] for t in range(tall)]
        picked.append(jnp.concatenate(tiles + [ends], axis=0))
    mixed = mm(jnp.concatenate(picked, axis=1), wt[...])
    top = tall * TILE
    part[0:top, :] = mixed[:top]
    part[top:channels, :] = sum(mixed[top + j * tail:top + (j + 1) * tail] for j in range(group))
    swap = remote(part, other, 9, partner)
    swap.start()
    swap.wait_recv()
    own = (part[...] + other[...]).astype(BF16)
    ext[1] = own
    rows_up()
    rows_down()

    gath[PAD:, :] = mm(own, hd[...]).astype(BF16)
    gown[...] = mm(own, hs[2 * nodes:, :]).astype(BF16)
    rows = ext[1, :, near_n].astype(F32).T.astype(BF16)
    inner = [mm(rows, mix[i, hid:]) for i in range(2)]
    first = mm(rows, embp[...]).astype(BF16)
    fin[...] = first
    swap.wait_send()
    rows_end_up()
    gown[...] = (gown[...].astype(F32) + mm(ext[2], hs[nodes:2 * nodes, :])).astype(BF16)
    rows_end_down()

    def pre_of(i):
        at = slice(i * CHUNK, (i + 1) * CHUNK)
        return mm(mt[...], gath[:, at])

    def edge_phase():
        gath[0:PAD, :] = (mm(ext[0], hs[0:nodes, :]) + gown[...].astype(F32)).astype(BF16)
        later = pre_of(0)
        for i in range(chunks):
            pre = later
            if i + 1 < chunks:
                later = pre_of(i + 1)
            hidden = silu_of_half(pre).astype(BF16)
            acc[...] += nt(hd[:, i * CHUNK:(i + 1) * CHUNK], hidden)

    edge_phase()

    give[...] = acc[far_n].astype(BF16)
    swap = remote(give, take, 10, partner)
    swap.start()
    swap.wait()
    total = (acc[near_n] + take[...].astype(F32)).astype(BF16)
    update = [silu_of_half(inner[i] + mm(total, mix[i, 0:hid])).astype(BF16) for i in range(2)]
    update = jnp.concatenate(update, axis=1)
    fin[:, theirs] = (fin[:, theirs].astype(F32) + mm(update, nout[:, theirs])).astype(BF16)
    last = remote(fin.at[:, theirs], out.at[near_n], 11, partner)
    last.start()
    out[near_n] = (fin[:, mine].astype(F32) + mm(update, nout[:, mine])).astype(BF16)
    last.wait()


def on_device(
    grid_field, band_points, block_ids, block_count, block_weight, embed_weight,
    edge_src, edge_dst, edge_in_weight, edge_out_weight, node_in_weight, node_out_weight,
):
    n = lax.axis_size("band")
    channels, points = grid_field.shape
    slots, nodes, block_len = block_weight.shape[1:]
    sub = points // block_len
    width = block_len // 2
    cols = embed_weight.shape[1]
    hid = 2 * cols
    edges = edge_src.shape[0] // 2
    bf = lambda *shape: pltpu.VMEM(shape, BF16)
    f32 = lambda *shape: pltpu.VMEM(shape, F32)
    return pl.pallas_call(
        functools.partial(layer_kernel, n),
        out_shape=pltpu.VMEM((nodes, cols), BF16),
        in_specs=[SMEM] * 2 + [HBM] * 10, out_specs=VMEM,
        scratch_shapes=[
            pltpu.SMEM((1, slots), jnp.int32),
            bf(sub, channels, width), bf(5 * channels * sub // 2 // TILE, TILE, width), bf(slots, nodes, width), bf(slots * width, nodes),
            bf(2, channels, cols), bf(PAD, hid), bf(hid, hid), bf(2, hid, cols), bf(2, hid, cols), bf(hid, hid),
            pltpu.VMEM((1, edges), jnp.int32), pltpu.VMEM((1, edges), jnp.int32),
            bf(hid, 2 * PAD), bf(2, hid + PAD, cols), bf(3 * nodes, edges), bf(nodes, edges),
            f32(PAD, nodes), f32(PAD, nodes), bf(3, PAD, nodes),
            bf(PAD, edges), bf(2 * PAD, edges), f32(nodes, hid),
            bf(nodes // 2, hid), bf(nodes // 2, hid), bf(nodes // 2, hid),
            pltpu.SemaphoreType.DMA, pltpu.SemaphoreType.DMA, pltpu.SemaphoreType.DMA, pltpu.SemaphoreType.DMA((7,)),
            pltpu.SemaphoreType.DMA((12,)), pltpu.SemaphoreType.DMA((12,)),
        ],
        compiler_params=pltpu.CompilerParams(vmem_limit_bytes=LARGE, collective_id=0, has_side_effects=True),
    )(
        block_count, band_points, *[pltpu.with_memory_space_constraint(x, pltpu.HBM) for x in (
            block_ids, grid_field, block_weight.reshape(block_weight.shape[1:]),
            embed_weight, edge_out_weight, edge_in_weight, node_in_weight, node_out_weight,
            edge_src.reshape(1, -1), edge_dst.reshape(1, -1),
        )],
    )


def solution(mesh):
    return jax.shard_map(
        on_device,
        mesh=mesh,
        in_specs=(
            P(None, "band"), P("band"), P("band", None), P("band"),
            P("band", None, None, None), P(None, "ch"), P("band"), P("band"),
            P(None, None, "ch"), P("ch", None), P(None, None, "ch"), P("ch", None),
        ),
        out_specs=P("band", "ch"),
        check_vma=False,
    )
```

```python
import functools

import jax
import jax.numpy as jnp
from jax import lax
from jax.experimental import pallas as pl
from jax.experimental.pallas import tpu as pltpu
from jax.sharding import PartitionSpec as P

MESH = pl.DeviceIdType.MESH
F32 = jnp.float32
BF16 = jnp.bfloat16
VMEM = pl.BlockSpec(memory_space=pltpu.VMEM)
SMEM = pl.BlockSpec(memory_space=pltpu.SMEM)
HBM = pl.BlockSpec(memory_space=pltpu.HBM)
LARGE = int(50 * 1024 * 1024)
CHUNK = 512
PAD = 128
ROWS = 104
TILE = 16


def nt(x, y):
    return lax.dot_general(x, y, (((1,), (1,)), ((), ())), preferred_element_type=F32)


def mm(x, y):
    return jnp.dot(x, y, preferred_element_type=F32)


def silu_of_half(v):
    return v + v * jnp.tanh(v)


def layer_kernel(
    n, count, live, ids_h, grid_h, w_h, emb_h, eo_h, win_h, nin_h, nout_h, src_h, dst_h, out,
    ids, raw, pool, wts, wt, emb, embp, eo, win, nin, nout, src, dst,
    mt, mix, hs, hd, part, other, ext, gown, gath, acc, give, take, fin,
    ssem, wsem, gsem, lsem, send, recv,
):
    b = lax.axis_index("band")
    c = lax.axis_index("ch")
    slots, nodes, block_len = w_h.shape
    width = block_len // 2
    channels = grid_h.shape[0]
    sub = grid_h.shape[1] // block_len
    half = sub // 2
    cols = emb_h.shape[1]
    hid = 2 * cols
    mine_e = src.shape[1]
    chunks = mine_e // CHUNK
    mid = nodes // 2
    tall = channels // TILE
    tail = channels % TILE
    group = TILE // tail
    quarter = (tall * half) + half // group
    up, down = jnp.minimum(b + 1, n - 1), jnp.maximum(b - 1, 0)
    has_up, has_down = b < n - 1, b > 0
    above, below, partner = (up, c), (down, c), (b, 1 - c)

    ext[...] = jnp.zeros_like(ext)
    barrier = pltpu.get_barrier_semaphore()

    @pl.when(has_up)
    def _():
        pl.semaphore_signal(barrier, inc=1, device_id=above, device_id_type=MESH)

    @pl.when(has_down)
    def _():
        pl.semaphore_signal(barrier, inc=1, device_id=below, device_id_type=MESH)

    pl.semaphore_signal(barrier, inc=1, device_id=partner, device_id_type=MESH)

    off = pl.multiple_of(c * width, width)
    gcopies = [
        pltpu.make_async_copy(
            grid_h.at[:, pl.ds(pl.multiple_of((2 * i + c) * width, width), width)], raw.at[i], gsem
        )
        for i in range(sub)
    ]
    names = pltpu.make_async_copy(ids_h, ids, ssem)
    for one in [names] + gcopies[half:] + gcopies[:half]:
        one.start()
    wcopy = pltpu.make_async_copy(w_h.at[:, :, pl.ds(off, width)], wts, wsem)
    mine = pl.ds(pl.multiple_of(c * cols, cols), cols)
    theirs = pl.ds(pl.multiple_of((1 - c) * cols, cols), cols)
    near_n = pl.ds(pl.multiple_of(c * mid, mid), mid)
    far_n = pl.ds(pl.multiple_of((1 - c) * mid, mid), mid)
    edges = pl.ds(pl.multiple_of(c * mine_e, mine_e), mine_e)
    local = [
        pltpu.make_async_copy(x, y, lsem.at[i])
        for i, (x, y) in enumerate(
            [(emb_h, emb.at[c]), (win_h, win), (eo_h, eo.at[mine]), (nin_h, nin), (nout_h, nout.at[mine]),
             (src_h.at[:, edges], src), (dst_h.at[:, edges], dst)]
        )
    ]

    def remote(source, target, k, device):
        return pltpu.make_async_remote_copy(
            src_ref=source, dst_ref=target, send_sem=send.at[k], recv_sem=recv.at[k],
            device_id=device, device_id_type=MESH,
        )

    def neighbours(fwd, bwd):
        def sends():
            pl.when(has_up)(fwd.wait_send)
            pl.when(has_down)(bwd.wait_send)

        return (
            lambda: pl.when(has_up)(fwd.start), lambda: pl.when(has_down)(bwd.start),
            lambda: pl.when(has_up)(bwd.wait_recv), lambda: pl.when(has_down)(fwd.wait_recv), sends,
        )

    halo_up, halo_down, halo_end_up, halo_end_down, halo_sends = neighbours(
        remote(pool.at[pl.ds(2 * quarter, quarter)], pool.at[pl.ds(0, quarter)], 0, above),
        remote(pool.at[pl.ds(quarter, quarter)], pool.at[pl.ds(3 * quarter, quarter)], 1, below),
    )
    sent = pl.ds(0, ROWS)
    rows_up, rows_down, rows_end_up, rows_end_down, rows_sends = neighbours(
        remote(ext.at[1, sent], ext.at[0, sent], 2, above), remote(ext.at[1, sent], ext.at[2, sent], 3, below)
    )
    weights = [
        remote(emb_h, emb.at[c], 4, partner), remote(eo_h, eo.at[mine], 5, partner),
        remote(nout_h, nout.at[mine], 6, partner),
    ]

    column = lax.broadcasted_iota(jnp.int32, (channels, width), 1) + c * width
    pltpu.make_async_copy(raw, raw, gsem).wait()
    names.wait()
    for i in range(0, sub, group):
        ends = []
        base, first_of = (1 + i // half) * quarter, i % half
        for j in range(group):
            block = raw[i + j]
            if i >= half:
                block = jnp.where(column < live[0] - (i + j) * block_len, block, jnp.zeros_like(block))
            for t in range(tall):
                pool[base + (first_of + j) * tall + t] = block[t * TILE:(t + 1) * TILE]
            ends.append(block[tall * TILE:].astype(F32))
        pool[base + tall * half + first_of // group] = jnp.concatenate(ends, axis=0).astype(BF16)
    pl.semaphore_wait(barrier, 1 + has_up.astype(jnp.int32) + has_down.astype(jnp.int32))
    halo_down()
    halo_up()
    for one in local + [wcopy] + weights:
        one.start()

    blank = jnp.zeros((quarter,) + pool.shape[1:], BF16)
    pool[4 * quarter:] = blank

    @pl.when(b == 0)
    def _():
        pool[0:quarter] = blank

    @pl.when(b == n - 1)
    def _():
        pool[3 * quarter:4 * quarter] = blank

    embp[...] = jnp.zeros_like(embp)
    acc[...] = jnp.zeros_like(acc)
    part[...] = jnp.zeros_like(part)
    other[ROWS:] = jnp.zeros((PAD - ROWS, nodes), F32)
    for one in local + weights:
        one.wait()
    embp[0:channels, 0:cols] = emb[0]
    embp[0:channels, cols:hid] = emb[1]
    for i in range(2):
        mixed = mm(embp[...], win[i]) * 0.5
        mt[mine, i * PAD:(i + 1) * PAD] = mixed.T.astype(BF16)
    mix[c, hid:] = (mm(embp[...], nin[0]) * 0.5).astype(BF16)
    mix[c, 0:hid] = (mm(eo[...], nin[1]) * 0.5).astype(BF16)
    shares = [
        remote(mt.at[mine], mt.at[mine], 7, partner), remote(mix.at[c], mix.at[c], 8, partner),
    ]
    for one in shares:
        one.start()

    def hot(i, carry):
        at = pl.ds(pl.multiple_of(i * CHUNK, CHUNK), CHUNK)
        s = src[:, at] - (b - 1) * nodes
        s = jnp.where(s < nodes, s, jnp.where(s < 2 * nodes, s + nodes, s - nodes))
        d = dst[:, at] - b * nodes
        hs[:, at] = jnp.where(lax.broadcasted_iota(jnp.int32, (3 * nodes, CHUNK), 0) == s, 1.0, 0.0).astype(BF16)
        hd[:, at] = jnp.where(lax.broadcasted_iota(jnp.int32, (nodes, CHUNK), 0) == d, 1.0, 0.0).astype(BF16)
        return carry

    lax.fori_loop(0, chunks, hot, 0)
    wcopy.wait()
    for k in range(slots):
        wt[k * width:(k + 1) * width, :] = wts[k].T
    for one in shares:
        one.wait()
    halo_end_up()
    halo_end_down()

    picked = []
    line = lax.broadcasted_iota(jnp.int32, (TILE, width), 0)
    for k in range(slots):
        rel = jnp.clip(ids[0, k] - b * sub + half, 0, 2 * sub - 1)
        part_of, i = rel // half, rel % half
        base = jnp.where(k < count[0], part_of, 4) * quarter
        low = i % group * tail
        ends = pool[base + tall * half + i // group]
        ends = jnp.where((line >= low) & (line < low + tail), ends, jnp.zeros_like(ends))
        tiles = [pool[base + i * tall + t] for t in range(tall)]
        picked.append(jnp.concatenate(tiles + [ends], axis=0))
    mixed = mm(jnp.concatenate(picked, axis=1), wt[...])
    top = tall * TILE
    part[0:top, :] = mixed[:top]
    part[top:channels, :] = sum(mixed[top + j * tail:top + (j + 1) * tail] for j in range(group))
    swap = remote(part.at[sent], other.at[sent], 9, partner)
    swap.start()
    swap.wait_recv()
    own = (part[...] + other[...]).astype(BF16)
    ext[1] = own
    rows_up()
    rows_down()

    gath[PAD:, :] = mm(own, hd[...]).astype(BF16)
    gown[...] = mm(own, hs[2 * nodes:, :]).astype(BF16)
    rows = ext[1, :, near_n].astype(F32).T.astype(BF16)
    inner = [mm(rows, mix[i, hid:]) for i in range(2)]
    first = mm(rows, embp[...]).astype(BF16)
    fin[...] = first
    rows_end_up()
    gown[...] = (gown[...].astype(F32) + mm(ext[2], hs[nodes:2 * nodes, :])).astype(BF16)
    rows_end_down()

    def pre_of(i):
        at = slice(i * CHUNK, (i + 1) * CHUNK)
        return mm(mt[...], gath[:, at])

    def edge_phase():
        gath[0:PAD, :] = (mm(ext[0], hs[0:nodes, :]) + gown[...].astype(F32)).astype(BF16)
        later = pre_of(0)
        for i in range(chunks):
            pre = later
            if i + 1 < chunks:
                later = pre_of(i + 1)
            hidden = silu_of_half(pre).astype(BF16)
            acc[...] += nt(hd[:, i * CHUNK:(i + 1) * CHUNK], hidden)

    edge_phase()

    give[...] = acc[far_n].astype(BF16)
    trade = remote(give, take, 10, partner)
    trade.start()
    swap.wait_send()
    halo_sends()
    rows_sends()
    trade.wait()
    total = (acc[near_n] + take[...].astype(F32)).astype(BF16)
    update = [silu_of_half(inner[i] + mm(total, mix[i, 0:hid])).astype(BF16) for i in range(2)]
    update = jnp.concatenate(update, axis=1)
    fin[:, theirs] = (fin[:, theirs].astype(F32) + mm(update, nout[:, theirs])).astype(BF16)
    last = remote(fin.at[:, theirs], out.at[near_n], 11, partner)
    last.start()
    out[near_n] = (fin[:, mine].astype(F32) + mm(update, nout[:, mine])).astype(BF16)
    last.wait()


def on_device(
    grid_field, band_points, block_ids, block_count, block_weight, embed_weight,
    edge_src, edge_dst, edge_in_weight, edge_out_weight, node_in_weight, node_out_weight,
):
    n = lax.axis_size("band")
    channels, points = grid_field.shape
    slots, nodes, block_len = block_weight.shape[1:]
    sub = points // block_len
    width = block_len // 2
    cols = embed_weight.shape[1]
    hid = 2 * cols
    edges = edge_src.shape[0] // 2
    bf = lambda *shape: pltpu.VMEM(shape, BF16)
    f32 = lambda *shape: pltpu.VMEM(shape, F32)
    return pl.pallas_call(
        functools.partial(layer_kernel, n),
        out_shape=pltpu.VMEM((nodes, cols), BF16),
        in_specs=[SMEM] * 2 + [HBM] * 10, out_specs=VMEM,
        scratch_shapes=[
            pltpu.SMEM((1, slots), jnp.int32),
            bf(sub, channels, width), bf(5 * channels * sub // 2 // TILE, TILE, width), bf(slots, nodes, width), bf(slots * width, nodes),
            bf(2, channels, cols), bf(PAD, hid), bf(hid, hid), bf(2, hid, cols), bf(2, hid, cols), bf(hid, hid),
            pltpu.VMEM((1, edges), jnp.int32), pltpu.VMEM((1, edges), jnp.int32),
            bf(hid, 2 * PAD), bf(2, hid + PAD, cols), bf(3 * nodes, edges), bf(nodes, edges),
            f32(PAD, nodes), f32(PAD, nodes), bf(3, PAD, nodes),
            bf(PAD, edges), bf(2 * PAD, edges), f32(nodes, hid),
            bf(nodes // 2, hid), bf(nodes // 2, hid), bf(nodes // 2, hid),
            pltpu.SemaphoreType.DMA, pltpu.SemaphoreType.DMA, pltpu.SemaphoreType.DMA, pltpu.SemaphoreType.DMA((7,)),
            pltpu.SemaphoreType.DMA((12,)), pltpu.SemaphoreType.DMA((12,)),
        ],
        compiler_params=pltpu.CompilerParams(vmem_limit_bytes=LARGE, collective_id=0, has_side_effects=True),
    )(
        block_count, band_points, *[pltpu.with_memory_space_constraint(x, pltpu.HBM) for x in (
            block_ids, grid_field, block_weight.reshape(block_weight.shape[1:]),
            embed_weight, edge_out_weight, edge_in_weight, node_in_weight, node_out_weight,
            edge_src.reshape(1, -1), edge_dst.reshape(1, -1),
        )],
    )


def solution(mesh):
    return jax.shard_map(
        on_device,
        mesh=mesh,
        in_specs=(
            P(None, "band"), P("band"), P("band", None), P("band"),
            P("band", None, None, None), P(None, "ch"), P("band"), P("band"),
            P(None, None, "ch"), P("ch", None), P(None, None, "ch"), P("ch", None),
        ),
        out_specs=P("band", "ch"),
        check_vma=False,
    )
```

```python
import functools

import jax
import jax.numpy as jnp
from jax import lax
from jax.experimental import pallas as pl
from jax.experimental.pallas import tpu as pltpu
from jax.sharding import PartitionSpec as P

MESH = pl.DeviceIdType.MESH
F32 = jnp.float32
BF16 = jnp.bfloat16
VMEM = pl.BlockSpec(memory_space=pltpu.VMEM)
SMEM = pl.BlockSpec(memory_space=pltpu.SMEM)
HBM = pl.BlockSpec(memory_space=pltpu.HBM)
LARGE = int(50 * 1024 * 1024)
CHUNK = 512
PAD = 128
ROWS = 104
TILE = 16


def nt(x, y):
    return lax.dot_general(x, y, (((1,), (1,)), ((), ())), preferred_element_type=F32)


def mm(x, y):
    return jnp.dot(x, y, preferred_element_type=F32)


def silu_of_half(v):
    return v + v * jnp.tanh(v)


def layer_kernel(
    n, count, live, ids_h, grid_h, w_h, emb_h, eo_h, win_h, nin_h, nout_h, src_h, dst_h, out,
    ids, raw, pool, wts, wt, emb, embp, eo, win, nin, nout, src, dst,
    mt, mix, hs, hd, part, other, ext, gown, gath, acc, give, take, fin,
    ssem, wsem, gsem, lsem, send, recv,
):
    b = lax.axis_index("band")
    c = lax.axis_index("ch")
    slots, nodes, block_len = w_h.shape
    width = block_len // 2
    channels = grid_h.shape[0]
    sub = grid_h.shape[1] // block_len
    half = sub // 2
    cols = emb_h.shape[1]
    hid = 2 * cols
    mine_e = src.shape[1]
    chunks = mine_e // CHUNK
    mid = nodes // 2
    tall = channels // TILE
    tail = channels % TILE
    group = TILE // tail
    quarter = (tall * half) + half // group
    up, down = jnp.minimum(b + 1, n - 1), jnp.maximum(b - 1, 0)
    has_up, has_down = b < n - 1, b > 0
    above, below, partner = (up, c), (down, c), (b, 1 - c)

    barrier = pltpu.get_barrier_semaphore()

    @pl.when(has_up)
    def _():
        pl.semaphore_signal(barrier, inc=1, device_id=above, device_id_type=MESH)

    @pl.when(has_down)
    def _():
        pl.semaphore_signal(barrier, inc=1, device_id=below, device_id_type=MESH)

    pl.semaphore_signal(barrier, inc=1, device_id=partner, device_id_type=MESH)

    off = pl.multiple_of(c * width, width)
    gcopies = [
        pltpu.make_async_copy(
            grid_h.at[:, pl.ds(pl.multiple_of((2 * i + c) * width, width), width)], raw.at[i], gsem
        )
        for i in range(sub)
    ]
    names = pltpu.make_async_copy(ids_h, ids, ssem)
    for one in [names] + gcopies[half:] + gcopies[:half]:
        one.start()
    wcopy = pltpu.make_async_copy(w_h.at[:, :, pl.ds(off, width)], wts, wsem)
    mine = pl.ds(pl.multiple_of(c * cols, cols), cols)
    theirs = pl.ds(pl.multiple_of((1 - c) * cols, cols), cols)
    near_n = pl.ds(pl.multiple_of(c * mid, mid), mid)
    far_n = pl.ds(pl.multiple_of((1 - c) * mid, mid), mid)
    edges = pl.ds(pl.multiple_of(c * mine_e, mine_e), mine_e)
    local = [
        pltpu.make_async_copy(x, y, lsem.at[i])
        for i, (x, y) in enumerate(
            [(emb_h, emb.at[c]), (win_h, win), (eo_h, eo.at[mine]), (nin_h, nin), (nout_h, nout.at[mine]),
             (src_h.at[:, edges], src), (dst_h.at[:, edges], dst)]
        )
    ]

    def remote(source, target, k, device):
        return pltpu.make_async_remote_copy(
            src_ref=source, dst_ref=target, send_sem=send.at[k], recv_sem=recv.at[k],
            device_id=device, device_id_type=MESH,
        )

    def neighbours(fwd, bwd):
        def sends():
            pl.when(has_up)(fwd.wait_send)
            pl.when(has_down)(bwd.wait_send)

        return (
            lambda: pl.when(has_up)(fwd.start), lambda: pl.when(has_down)(bwd.start),
            lambda: pl.when(has_up)(bwd.wait_recv), lambda: pl.when(has_down)(fwd.wait_recv), sends,
        )

    halo_up, halo_down, halo_end_up, halo_end_down, halo_sends = neighbours(
        remote(pool.at[pl.ds(2 * quarter, quarter)], pool.at[pl.ds(0, quarter)], 0, above),
        remote(pool.at[pl.ds(quarter, quarter)], pool.at[pl.ds(3 * quarter, quarter)], 1, below),
    )
    sent = pl.ds(0, ROWS)
    rows_up, rows_down, rows_end_up, rows_end_down, rows_sends = neighbours(
        remote(ext.at[1, sent], ext.at[0, sent], 2, above), remote(ext.at[1, sent], ext.at[2, sent], 3, below)
    )
    weights = [
        remote(emb_h, emb.at[c], 4, partner), remote(eo_h, eo.at[mine], 5, partner),
        remote(nout_h, nout.at[mine], 6, partner),
    ]

    column = lax.broadcasted_iota(jnp.int32, (channels, width), 1) + c * width
    pltpu.make_async_copy(raw, raw, gsem).wait()
    names.wait()
    for i in range(0, sub, group):
        ends = []
        base, first_of = (1 + i // half) * quarter, i % half
        for j in range(group):
            block = raw[i + j]
            if i >= half:
                block = jnp.where(column < live[0] - (i + j) * block_len, block, jnp.zeros_like(block))
            for t in range(tall):
                pool[base + (first_of + j) * tall + t] = block[t * TILE:(t + 1) * TILE]
            ends.append(block[tall * TILE:].astype(F32))
        pool[base + tall * half + first_of // group] = jnp.concatenate(ends, axis=0).astype(BF16)
    pl.semaphore_wait(barrier, 1 + has_up.astype(jnp.int32) + has_down.astype(jnp.int32))
    halo_down()
    halo_up()
    for one in local + [wcopy] + weights:
        one.start()

    blank = jnp.zeros((quarter,) + pool.shape[1:], BF16)
    pool[4 * quarter:] = blank

    @pl.when(b == 0)
    def _():
        pool[0:quarter] = blank
        ext[0, 0:ROWS] = jnp.zeros((ROWS, nodes), BF16)

    @pl.when(b == n - 1)
    def _():
        pool[3 * quarter:4 * quarter] = blank
        ext[2, 0:ROWS] = jnp.zeros((ROWS, nodes), BF16)

    embp[...] = jnp.zeros_like(embp)
    acc[...] = jnp.zeros_like(acc)
    part[...] = jnp.zeros_like(part)
    ext[:, ROWS:] = jnp.zeros((3, PAD - ROWS, nodes), BF16)
    other[ROWS:] = jnp.zeros((PAD - ROWS, nodes), F32)
    for one in local + weights:
        one.wait()
    embp[0:channels, 0:cols] = emb[0]
    embp[0:channels, cols:hid] = emb[1]
    for i in range(2):
        mixed = mm(embp[...], win[i]) * 0.5
        mt[mine, i * PAD:(i + 1) * PAD] = mixed.T.astype(BF16)
    mix[c, hid:] = (mm(embp[...], nin[0]) * 0.5).astype(BF16)
    mix[c, 0:hid] = (mm(eo[...], nin[1]) * 0.5).astype(BF16)
    shares = [
        remote(mt.at[mine], mt.at[mine], 7, partner), remote(mix.at[c], mix.at[c], 8, partner),
    ]
    for one in shares:
        one.start()

    def hot(i, carry):
        at = pl.ds(pl.multiple_of(i * CHUNK, CHUNK), CHUNK)
        s = src[:, at] - (b - 1) * nodes
        s = jnp.where(s < nodes, s, jnp.where(s < 2 * nodes, s + nodes, s - nodes))
        d = dst[:, at] - b * nodes
        hs[:, at] = jnp.where(lax.broadcasted_iota(jnp.int32, (3 * nodes, CHUNK), 0) == s, 1.0, 0.0).astype(BF16)
        hd[:, at] = jnp.where(lax.broadcasted_iota(jnp.int32, (nodes, CHUNK), 0) == d, 1.0, 0.0).astype(BF16)
        return carry

    lax.fori_loop(0, chunks, hot, 0)
    wcopy.wait()
    for k in range(slots):
        wt[k * width:(k + 1) * width, :] = wts[k].T
    for one in shares:
        one.wait()
    halo_end_up()
    halo_end_down()

    picked = []
    line = lax.broadcasted_iota(jnp.int32, (TILE, width), 0)
    for k in range(slots):
        rel = jnp.clip(ids[0, k] - b * sub + half, 0, 2 * sub - 1)
        part_of, i = rel // half, rel % half
        base = jnp.where(k < count[0], part_of, 4) * quarter
        low = i % group * tail
        ends = pool[base + tall * half + i // group]
        ends = jnp.where((line >= low) & (line < low + tail), ends, jnp.zeros_like(ends))
        tiles = [pool[base + i * tall + t] for t in range(tall)]
        picked.append(jnp.concatenate(tiles + [ends], axis=0))
    mixed = mm(jnp.concatenate(picked, axis=1), wt[...])
    top = tall * TILE
    part[0:top, :] = mixed[:top]
    part[top:channels, :] = sum(mixed[top + j * tail:top + (j + 1) * tail] for j in range(group))
    swap = remote(part.at[sent], other.at[sent], 9, partner)
    swap.start()
    swap.wait_recv()
    own = (part[...] + other[...]).astype(BF16)
    ext[1] = own
    rows_up()
    rows_down()

    gath[PAD:, :] = mm(own, hd[...]).astype(BF16)
    gown[...] = mm(own, hs[2 * nodes:, :]).astype(BF16)
    rows = ext[1, :, near_n].astype(F32).T.astype(BF16)
    inner = [mm(rows, mix[i, hid:]) for i in range(2)]
    first = mm(rows, embp[...]).astype(BF16)
    fin[...] = first
    rows_end_up()
    gown[...] = (gown[...].astype(F32) + mm(ext[2], hs[nodes:2 * nodes, :])).astype(BF16)
    rows_end_down()

    def pre_of(i):
        at = slice(i * CHUNK, (i + 1) * CHUNK)
        return mm(mt[...], gath[:, at])

    def edge_phase():
        gath[0:PAD, :] = (mm(ext[0], hs[0:nodes, :]) + gown[...].astype(F32)).astype(BF16)
        later = pre_of(0)
        for i in range(chunks):
            pre = later
            if i + 1 < chunks:
                later = pre_of(i + 1)
            hidden = silu_of_half(pre).astype(BF16)
            acc[...] += nt(hd[:, i * CHUNK:(i + 1) * CHUNK], hidden)

    edge_phase()

    give[...] = acc[far_n].astype(BF16)
    trade = remote(give, take, 10, partner)
    trade.start()
    swap.wait_send()
    halo_sends()
    rows_sends()
    trade.wait()
    total = (acc[near_n] + take[...].astype(F32)).astype(BF16)
    update = [silu_of_half(inner[i] + mm(total, mix[i, 0:hid])).astype(BF16) for i in range(2)]
    update = jnp.concatenate(update, axis=1)
    fin[:, theirs] = (fin[:, theirs].astype(F32) + mm(update, nout[:, theirs])).astype(BF16)
    last = remote(fin.at[:, theirs], out.at[near_n], 11, partner)
    last.start()
    out[near_n] = (fin[:, mine].astype(F32) + mm(update, nout[:, mine])).astype(BF16)
    last.wait()


def on_device(
    grid_field, band_points, block_ids, block_count, block_weight, embed_weight,
    edge_src, edge_dst, edge_in_weight, edge_out_weight, node_in_weight, node_out_weight,
):
    n = lax.axis_size("band")
    channels, points = grid_field.shape
    slots, nodes, block_len = block_weight.shape[1:]
    sub = points // block_len
    width = block_len // 2
    cols = embed_weight.shape[1]
    hid = 2 * cols
    edges = edge_src.shape[0] // 2
    bf = lambda *shape: pltpu.VMEM(shape, BF16)
    f32 = lambda *shape: pltpu.VMEM(shape, F32)
    return pl.pallas_call(
        functools.partial(layer_kernel, n),
        out_shape=pltpu.VMEM((nodes, cols), BF16),
        in_specs=[SMEM] * 2 + [HBM] * 10, out_specs=VMEM,
        scratch_shapes=[
            pltpu.SMEM((1, slots), jnp.int32),
            bf(sub, channels, width), bf(5 * channels * sub // 2 // TILE, TILE, width), bf(slots, nodes, width), bf(slots * width, nodes),
            bf(2, channels, cols), bf(PAD, hid), bf(hid, hid), bf(2, hid, cols), bf(2, hid, cols), bf(hid, hid),
            pltpu.VMEM((1, edges), jnp.int32), pltpu.VMEM((1, edges), jnp.int32),
            bf(hid, 2 * PAD), bf(2, hid + PAD, cols), bf(3 * nodes, edges), bf(nodes, edges),
            f32(PAD, nodes), f32(PAD, nodes), bf(3, PAD, nodes),
            bf(PAD, edges), bf(2 * PAD, edges), f32(nodes, hid),
            bf(nodes // 2, hid), bf(nodes // 2, hid), bf(nodes // 2, hid),
            pltpu.SemaphoreType.DMA, pltpu.SemaphoreType.DMA, pltpu.SemaphoreType.DMA, pltpu.SemaphoreType.DMA((7,)),
            pltpu.SemaphoreType.DMA((12,)), pltpu.SemaphoreType.DMA((12,)),
        ],
        compiler_params=pltpu.CompilerParams(vmem_limit_bytes=LARGE, collective_id=0, has_side_effects=True),
    )(
        block_count, band_points, *[pltpu.with_memory_space_constraint(x, pltpu.HBM) for x in (
            block_ids, grid_field, block_weight.reshape(block_weight.shape[1:]),
            embed_weight, edge_out_weight, edge_in_weight, node_in_weight, node_out_weight,
            edge_src.reshape(1, -1), edge_dst.reshape(1, -1),
        )],
    )


def solution(mesh):
    return jax.shard_map(
        on_device,
        mesh=mesh,
        in_specs=(
            P(None, "band"), P("band"), P("band", None), P("band"),
            P("band", None, None, None), P(None, "ch"), P("band"), P("band"),
            P(None, None, "ch"), P("ch", None), P(None, None, "ch"), P("ch", None),
        ),
        out_specs=P("band", "ch"),
        check_vma=False,
    )
```
